256 devices in a mesh: gx: 32 (over z_hi, y, core), gy: 8 (over x, z_lo).
Axes of the slice: x: 4, y: 4, z: 8 (z_hi: 4, z_lo: 2; z = z_hi * 2 + z_lo), core: 2. Of those that a mesh axis runs over, the one named last changes fastest.
Arguments:
- state: float32 [12, 256, 16, 2048], P(None, 'gx', None, 'gy'), may hold values from -0.9 to 1, as said below
- tissue_mask: int32 [256, 16, 16], P('gx', None, 'gy'), may hold values 0 or 1
- layer_index: int32 [16], replicated, may hold values from 0 to 7
- fibre: float32 [2, 8], replicated, may hold values from -1.2 to 1.2
Outputs:
- new_state: float32 [12, 256, 16, 2048], P(None, 'gx', None, 'gy')
The draws below stay inside these ranges and needn't reach their ends.
Inputs may be any that keep to these rules, and one draw needn't show every extreme that they name: `state`: component 0 lies within -0.9 to 0.3, components 1 to 10 within 0 to 1, component 11 within 0.05 to 1.
All inputs are finite; a program needn't handle non-finite values.
Results may differ from the reference program's by a relative error of at most 0.00002.
Values sent between devices are 32-bit elements.
A program may use at most 64 MiB of HBM per device.

```python
import math
import jax
import jax.numpy as jnp
from jax import lax

NZ = 16
STEPS = 8
LAYERS = 8
COMPS = 12
MASK_BLOCK = 128
NX = 256
NY = 2048


def draw_state(key, part):
    keys = jax.random.split(jax.random.fold_in(key, 17), 3)
    gates_shape = (COMPS - 2, NX, NZ, NY)
    cell_shape = (1, NX, NZ, NY)
    voltage = jax.random.uniform(keys[0], cell_shape, jnp.float32, -0.9, 0.3)
    gates = jax.random.uniform(keys[1], gates_shape, jnp.float32)
    calcium = 0.05 * 20.0 ** jax.random.uniform(keys[2], cell_shape, jnp.float32)
    return jnp.concatenate([voltage, gates, calcium], axis=0).astype(jnp.float32)


def place_ends(values, key, least, largest):
    index_at = [jax.random.randint(jax.random.fold_in(key, axis), (), 0, length) for axis, length in enumerate(values.shape)]
    longest = values.shape.index(max(values.shape))
    beside = index_at[:longest] + [(index_at[longest] + 1) % values.shape[longest]] + index_at[longest + 1:]
    return values.at[tuple(index_at)].set(least).at[tuple(beside)].set(largest)


def setup_inputs(seed: int = 0) -> dict:
    streams_of = jax.random.split(jax.random.key(seed), 5)
    return {
        "state": draw_state(jax.random.fold_in(streams_of[4], 71), 0),
        "tissue_mask": place_ends((jax.random.randint(streams_of[1], (NX, NZ, NY // MASK_BLOCK), 0, 4) < 3).astype(jnp.int32), jax.random.fold_in(streams_of[1], 1), 0, 1),
        "layer_index": place_ends(jax.random.randint(streams_of[2], (NZ,), 0, LAYERS), jax.random.fold_in(streams_of[2], 1), 0, LAYERS - 1).astype(jnp.int32),
        "fibre": jnp.clip(jax.random.uniform(streams_of[3], (2, LAYERS), jnp.float32, -1.2, 1.2), -1.2, 1.2),
    }


time_step = 0.02
thermal_volt = 8314.472 * 310.0 / 96485.3415
potassium_out = 5.4
sodium_out = 140.0
calcium_out = 2.0
potassium_in = 138.3
sodium_in = 7.67
transverse = 0.04
longitudinal = 0.12

def settle(gate, steady, tau):
    return steady + (gate - steady) * jnp.exp(-time_step / tau)

def settle_rate(gate, steady, rate):
    return steady + (gate - steady) * jnp.exp(-time_step * rate)

def membrane(state):
    sig = jax.nn.sigmoid
    voltage = 100.0 * state[0]
    sodium_act = state[1]
    sodium_inact = state[2]
    sodium_slow = state[3]
    calcium_act = state[4]
    calcium_inact = state[5]
    transient_act = state[6]
    transient_inact = state[7]
    rapid_act = state[8]
    rapid_inact = state[9]
    slow_act = state[10]
    calcium = state[11]
    calcium_mm = jnp.maximum(calcium, 0.02) * 0.001
    rev_potassium = thermal_volt * math.log(potassium_out / potassium_in)
    rev_sodium = thermal_volt * math.log(sodium_out / sodium_in)
    rev_slow = thermal_volt * math.log((potassium_out + 0.03 * sodium_out) / (potassium_in + 0.03 * sodium_in))
    rev_calcium = 0.5 * thermal_volt * jnp.log(calcium_out / calcium_mm)
    sodium_current = 14.838 * sodium_act ** 3 * sodium_inact * sodium_slow * (voltage - rev_sodium)
    calcium_current = 0.08 * calcium_act * calcium_inact * (voltage - rev_calcium)
    transient_current = 0.294 * transient_act * transient_inact * (voltage - rev_potassium)
    rapid_current = 0.153 * rapid_act * rapid_inact * (voltage - rev_potassium)
    slow_current = 0.392 * slow_act ** 2 * (voltage - rev_slow)
    above = voltage - rev_potassium
    alpha_inward = 0.1 * sig(-0.06 * (above - 200.0))
    beta_inward = (3.0 * jnp.exp(0.0002 * (above + 100.0)) + jnp.exp(0.1 * (above - 10.0))) * sig(0.5 * above)
    inward_current = 5.405 * alpha_inward / (alpha_inward + beta_inward) * above
    plateau_current = 0.0146 * sig((voltage - 25.0) / 5.98) * above
    scaled = voltage / thermal_volt
    pump_current = 2.724 * potassium_out / (potassium_out + 1.0) * sodium_in / (sodium_in + 40.0) / (1.0 + 0.1245 * jnp.exp(-0.1 * scaled) + 0.0353 * jnp.exp(-scaled))
    exchange_current = 1000.0 * (jnp.exp(0.35 * scaled) * sodium_in ** 3 * calcium_out - 2.5 * jnp.exp(-0.65 * scaled) * sodium_out ** 3 * calcium_mm) / ((87.5 ** 3 + sodium_out ** 3) * (1.38 + calcium_out) * (1.0 + 0.1 * jnp.exp(-0.65 * scaled)))
    pump_calcium = 0.1238 * calcium_mm / (calcium_mm + 0.0005)
    back_sodium = 0.00029 * (voltage - rev_sodium)
    back_calcium = 0.000592 * (voltage - rev_calcium)
    ionic_total = sodium_current + calcium_current + transient_current + rapid_current + slow_current + inward_current + plateau_current + pump_current + exchange_current + pump_calcium + back_sodium + back_calcium
    new_voltage = voltage - time_step * ionic_total
    new_calcium = calcium - time_step * 0.05 * (calcium_current + back_calcium + pump_calcium - 2.0 * exchange_current)
    upper = sig((voltage + 40.0) / 2.0)
    lower = sig(-(voltage + 40.0) / 2.0)
    tau_act = sig((voltage + 60.0) / 5.0) * (0.1 * sig(-(voltage + 35.0) / 5.0) + 0.1 * sig(-(voltage - 50.0) / 200.0))
    new_act = settle(sodium_act, sig((voltage + 56.86) / 9.03) ** 2, tau_act)
    inact_steady = sig(-(voltage + 71.55) / 7.43) ** 2
    rate_inact = lower * 0.057 * jnp.exp(-(voltage + 80.0) / 6.8) + upper * (0.77 / 0.13) * sig((voltage + 10.66) / 11.1) + lower * (2.7 * jnp.exp(0.079 * voltage) + 310000.0 * jnp.exp(0.3485 * voltage))
    new_inact = settle_rate(sodium_inact, inact_steady, rate_inact)
    rate_slow = lower * (-25428.0 * jnp.exp(0.2444 * voltage) - 6.948e-06 * jnp.exp(-0.04391 * voltage)) * (voltage + 37.78) * sig(-0.311 * (voltage + 79.23)) + lower * 0.02424 * jnp.exp(-0.01052 * voltage) * sig(0.1378 * (voltage + 40.14)) + upper * 0.6 * jnp.exp(0.057 * voltage) * sig(0.1 * (voltage + 32.0))
    new_slow = settle_rate(sodium_slow, inact_steady, rate_slow)
    tau_calact = (1.4 * sig((voltage + 35.0) / 13.0) + 0.25) * 1.4 * sig(-(voltage + 5.0) / 5.0) + sig((voltage - 50.0) / 20.0)
    new_calact = settle(calcium_act, sig((voltage + 8.0) / 7.5), tau_calact)
    tau_calinact = 1102.5 * jnp.exp(-(voltage + 27.0) ** 2 / 225.0) + 200.0 * sig((voltage - 13.0) / 10.0) + 180.0 * sig(-(voltage + 30.0) / 10.0) + 20.0
    new_calinact = settle(calcium_inact, sig(-(voltage + 20.0) / 7.0), tau_calinact)
    tau_tract = 9.5 * jnp.exp(-(voltage + 40.0) ** 2 / 1800.0) + 0.8
    new_tract = settle(transient_act, sig((voltage - 20.0) / 6.0), tau_tract)
    tau_trinact = 85.0 * jnp.exp(-(voltage + 45.0) ** 2 / 320.0) + 5.0 * sig(-(voltage - 20.0) / 5.0) + 3.0
    new_trinact = settle(transient_inact, sig(-(voltage + 20.0) / 5.0), tau_trinact)
    tau_rapact = 450.0 * sig((voltage + 45.0) / 10.0) * 6.0 * sig(-(voltage + 30.0) / 11.5)
    new_rapact = settle(rapid_act, sig((voltage + 26.0) / 7.0), tau_rapact)
    tau_rapinact = 3.0 * sig((voltage + 60.0) / 20.0) * 1.12 * sig(-(voltage - 60.0) / 20.0)
    new_rapinact = settle(rapid_inact, sig(-(voltage + 88.0) / 24.0), tau_rapinact)
    tau_slowact = 1400.0 * jnp.sqrt(sig((voltage - 5.0) / 6.0)) * sig(-(voltage - 35.0) / 15.0) + 80.0
    new_slowact = settle(slow_act, sig((voltage + 5.0) / 14.0), tau_slowact)
    return jnp.stack([new_voltage / 100.0, new_act, new_inact, new_slow, new_calact, new_calinact, new_tract, new_trinact, new_rapact, new_rapinact, new_slowact, new_calcium])

def advance(state, inside):
    return jnp.where(inside[None], membrane(state), state)

def layer_tensor(layer_index, fibre):
    angle_in = fibre[0]
    angle_out = fibre[1]
    fibre_x = jnp.cos(angle_in) * jnp.cos(angle_out)
    fibre_y = jnp.sin(angle_in) * jnp.cos(angle_out)
    fibre_z = jnp.sin(angle_out)
    spread = longitudinal - transverse
    tensor_table = jnp.stack([transverse + spread * fibre_x * fibre_x, transverse + spread * fibre_y * fibre_y, transverse + spread * fibre_z * fibre_z, spread * fibre_x * fibre_y, spread * fibre_x * fibre_z, spread * fibre_y * fibre_z])
    layer_ids = jnp.arange(fibre.shape[1], dtype=jnp.int32)
    chosen = layer_index[:, None] == layer_ids[None, :]
    return lax.optimization_barrier(jnp.sum(jnp.where(chosen[None], tensor_table[:, None, :], jnp.float32(0.0)), axis=2))

def weights(tensor, offset_x, offset_y, offset_z):
    if offset_z == 0:
        if offset_x != 0 and offset_y != 0:
            return offset_x * offset_y * tensor[3] / 2.0
        if offset_x != 0:
            return tensor[0]
        return tensor[1]
    extent_z = tensor.shape[1]
    padded_tensor = jnp.pad(tensor, ((0, 0), (1, 1)), mode='edge')
    averaged = (tensor + padded_tensor[:, 1 + offset_z:1 + offset_z + extent_z]) / 2.0
    if offset_x == 0 and offset_y == 0:
        return averaged[2]
    if offset_x != 0:
        return offset_x * offset_z * averaged[4] / 2.0
    return offset_y * offset_z * averaged[5] / 2.0

def stencil(volt_shell, mask_shell, tensor):
    volt_padded = jnp.pad(volt_shell, ((0, 0), (1, 1), (0, 0)))
    mask_padded = jnp.pad(mask_shell, ((0, 0), (1, 1), (0, 0)))
    extent_x = volt_shell.shape[0] - 2
    extent_z = volt_shell.shape[1]
    extent_y = volt_shell.shape[2] - 2
    centre = volt_padded[1:1 + extent_x, 1:1 + extent_z, 1:1 + extent_y]
    mask_centre = mask_padded[1:1 + extent_x, 1:1 + extent_z, 1:1 + extent_y]
    flux_sum = jnp.zeros_like(centre)
    for offset_x in (-1, 0, 1):
        for offset_y in (-1, 0, 1):
            for offset_z in (-1, 0, 1):
                length = offset_x * offset_x + offset_y * offset_y + offset_z * offset_z
                if length == 0 or length > 2:
                    continue
                weight = weights(tensor, offset_x, offset_y, offset_z)[None, :, None]
                neighbour = volt_padded[1 + offset_x:1 + offset_x + extent_x, 1 + offset_z:1 + offset_z + extent_z, 1 + offset_y:1 + offset_y + extent_y]
                mask_near = mask_padded[1 + offset_x:1 + offset_x + extent_x, 1 + offset_z:1 + offset_z + extent_z, 1 + offset_y:1 + offset_y + extent_y]
                flux_sum = flux_sum + weight * mask_near * (neighbour - centre)
    return mask_centre * flux_sum

def expand_mask(blocks):
    cells_x, extent_z, block_count = blocks.shape
    spread = jnp.broadcast_to(blocks[:, :, :, None], (cells_x, extent_z, block_count, MASK_BLOCK))
    return spread.reshape(cells_x, extent_z, block_count * MASK_BLOCK) > 0

def reference(state, tissue_mask, layer_index, fibre):
    tensor = layer_tensor(layer_index, fibre)
    inside = expand_mask(tissue_mask)
    mask_shell = jnp.pad(inside.astype(jnp.float32), ((1, 1), (0, 0), (1, 1)))
    column_state = jnp.moveaxis(state, 1, 0)
    for repeat in range(STEPS):
        reacted = lax.map(lambda paired: advance(paired[0], paired[1]), (column_state, inside))
        voltage = reacted[:, 0]
        volt_shell = jnp.pad(voltage, ((1, 1), (0, 0), (1, 1)))
        column_state = reacted.at[:, 0].set(voltage + stencil(volt_shell, mask_shell, tensor))
    return jnp.moveaxis(column_state, 0, 1)
```

```python
import math

import jax
import jax.numpy as jnp
from jax import lax
from jax.experimental import pallas as pl
from jax.experimental.pallas import tpu as pltpu
from jax.sharding import PartitionSpec as P

STEPS = 8
TRANSVERSE = 0.04
LONGITUDINAL = 0.12
DT = 0.02
RTF = 8314.472 * 310.0 / 96485.3415
EK = RTF * math.log(5.4 / 138.3)
ENA = RTF * math.log(140.0 / 7.67)
EKS = RTF * math.log((5.4 + 0.03 * 140.0) / (138.3 + 0.03 * 7.67))
L2E = 1.0 / math.log(2.0)
KAPPA = -DT * L2E


def grow(volt, slope):
    return jnp.exp2(volt * (slope * L2E))


def sig(volt, centre, width):
    return jax.nn.sigmoid(volt * (1.0 / width) + (-centre / width))


def settle(gate, steady, factor):
    return steady + (gate - steady) * jnp.exp2(factor)


def membrane(s):
    x, m, h, j, d, f, r, z, p, q, w, ca = s
    v = x * 100.0
    over = v - EK
    b = grow(v, 0.05)
    ib = 1.0 / b
    b2 = b * b
    ib2 = ib * ib
    c = jnp.maximum(ca, 0.02)
    vca = (v - 0.5 * RTF * math.log(2000.0)) + (0.5 * RTF) * jnp.log(c)
    sodium = ((14.838 * m) * (m * m) * (h * j) + 0.00029) * (v - ENA)
    calcium = (0.08 * d * f + 0.000592) * vca
    sa = sig(v, EK + 200.0, -1.0 / 0.06)
    bk = (
        (30.0 * math.exp(0.0002 * (100.0 - EK))) * grow(v, 0.0002)
        + (10.0 * math.exp(0.1 * (-EK - 10.0))) * b2
    ) * sig(v, EK, 2.0)
    inward = 5.405 * sa / (sa + bk)
    potassium = (
        0.294 * r * z + 0.153 * p * q + inward + 0.0146 * sig(v, 25.0, 5.98)
    ) * over
    slow = (0.392 * w) * w * (v - EKS)
    en = grow(v, -1.0 / RTF)
    pump = (2.724 * 5.4 / 6.4 * 7.67 / 47.67) / (
        1.0 + 0.1245 * grow(v, -0.1 / RTF) + 0.0353 * en
    )
    ef = grow(v, 0.35 / RTF)
    eg = ef * en
    scale = 1000.0 / ((87.5**3 + 140.0**3) * 3.38)
    exchange = (
        (scale * 7.67**3 * 2.0) * ef - (scale * 2.5 * 140.0**3 * 0.001) * eg * c
    ) / (1.0 + 0.1 * eg)
    pump_ca = 0.1238 * c / (c + 0.5)
    total = sodium + calcium + potassium + slow + pump + exchange + pump_ca
    nx = x - (DT / 100.0) * total
    nca = ca - (DT * 0.05) * (calcium + pump_ca - 2.0 * exchange)
    low = 1.0 / (1.0 + math.exp(20.0) * grow(v, 0.5))
    nm = settle(
        m,
        sig(v, -56.86, 9.03) ** 2,
        (10.0 * KAPPA + (10.0 * KAPPA * math.exp(-12.0)) * (ib2 * ib2))
        / (sig(v, -35.0, -5.0) + sig(v, 50.0, -200.0)),
    )
    hs = sig(v, -71.55, -7.43)
    hs = hs * hs
    up = (KAPPA * 0.77 / 0.13) * sig(v, -10.66, 11.1)
    dn = (
        (KAPPA * 0.057 * math.exp(-80.0 / 6.8)) * grow(v, -1.0 / 6.8)
        + (KAPPA * 2.7) * grow(v, 0.079)
        + (KAPPA * 310000.0) * grow(v, 0.3485)
    )
    nh = settle(h, hs, up + low * (dn - up))
    up = (KAPPA * 0.6) * grow(v, 0.057) * sig(v, -32.0, 10.0)
    dn = ((KAPPA * -25428.0) * grow(v, 0.2444) - (KAPPA * 6.948e-06) * grow(v, -0.04391)) * (
        v + 37.78
    ) * sig(v, -79.23, -1.0 / 0.311) + (KAPPA * 0.02424) * grow(v, -0.01052) * sig(
        v, -40.14, 1.0 / 0.1378
    )
    nj = settle(j, hs, up + low * (dn - up))
    nd = settle(
        d,
        sig(v, -8.0, 7.5),
        KAPPA
        / ((1.96 * sig(v, -35.0, 13.0) + 0.35) * sig(v, -5.0, -5.0) + sig(v, 50.0, 20.0)),
    )
    t = v + 27.0
    nf = settle(
        f,
        sig(v, -20.0, -7.0),
        1.0
        / (
            (1102.5 / KAPPA) * jnp.exp2(t * t * (-L2E / 225.0))
            + (200.0 / KAPPA) * sig(v, 13.0, 10.0)
            + (180.0 / KAPPA) * sig(v, -30.0, -10.0)
            + 20.0 / KAPPA
        ),
    )
    t = v + 40.0
    nr = settle(
        r,
        sig(v, 20.0, 6.0),
        1.0 / ((9.5 / KAPPA) * jnp.exp2(t * t * (-L2E / 1800.0)) + 0.8 / KAPPA),
    )
    t = v + 45.0
    nz = settle(
        z,
        sig(v, -20.0, -5.0),
        1.0
        / (
            (85.0 / KAPPA) * jnp.exp2(t * t * (-L2E / 320.0))
            + (5.0 / KAPPA) * sig(v, 20.0, -5.0)
            + 3.0 / KAPPA
        ),
    )
    k = KAPPA / 2700.0
    np_ = settle(
        p,
        sig(v, -26.0, 7.0),
        (k + (k * math.exp(-4.5)) * ib2)
        * (1.0 + math.exp(30.0 / 11.5) * grow(v, 1.0 / 11.5)),
    )
    k = KAPPA / 3.36
    nq = settle(
        q,
        sig(v, -88.0, -24.0),
        (k * (1.0 + math.exp(-6.0))) + (k * math.exp(-3.0)) * (b + ib),
    )
    nw = settle(
        w,
        sig(v, -5.0, 14.0),
        1.0
        / (
            lax.rsqrt(1.0 + math.exp(5.0 / 6.0) * grow(v, -1.0 / 6.0))
            * ((1400.0 / KAPPA) * sig(v, 35.0, -15.0))
            + 80.0 / KAPPA
        ),
    )
    return nx, nm, nh, nj, nd, nf, nr, nz, np_, nq, nw, nca


INNER = 8
COMPS = 12
HOPS = STEPS - 1
MESH = pl.DeviceIdType.MESH


def react(state, inside):
    fresh = membrane(state)
    return [jnp.where(inside, new, old) for new, old in zip(fresh, state)]


def lanes():
    return lax.broadcasted_iota(jnp.int32, (16, 128), 1)


def turn(tile, shift):
    shift = shift % 128
    return tile if shift == 0 else pltpu.roll(tile, shift, 1)


def coefficients(layer_ref, fibre_ref, coef):
    row = lax.broadcasted_iota(jnp.int32, (16, 128), 0)
    angle_in = jnp.zeros((16, 128), jnp.float32)
    angle_out = jnp.zeros((16, 128), jnp.float32)
    for level in range(16):
        layer = layer_ref[level]
        angle_in = jnp.where(row == level, fibre_ref[0, layer], angle_in)
        angle_out = jnp.where(row == level, fibre_ref[1, layer], angle_out)
    along_x = jnp.cos(angle_in) * jnp.cos(angle_out)
    along_y = jnp.sin(angle_in) * jnp.cos(angle_out)
    along_z = jnp.sin(angle_out)
    spread = LONGITUDINAL - TRANSVERSE
    coef[0] = TRANSVERSE + spread * along_x * along_x
    coef[1] = TRANSVERSE + spread * along_y * along_y
    coef[2] = spread * along_x * along_y / 2.0
    parts = (
        TRANSVERSE + spread * along_z * along_z,
        spread * along_x * along_z / 2.0,
        spread * along_y * along_z / 2.0,
    )
    for index, part in enumerate(parts):
        below = (part + pltpu.roll(part, 1, 0)) / 2.0
        above = (part + pltpu.roll(part, 15, 0)) / 2.0
        coef[3 + index] = jnp.where(row == 0, 0.0, below)
        coef[6 + index] = jnp.where(row == 15, 0.0, above)


def tile_sum(coef, here, up, down):
    value, both, slope = here
    across = up[0] - down[0]
    rising = coef[3] * value + coef[4] * across + coef[5] * slope
    falling = coef[6] * value - coef[7] * across - coef[8] * slope
    flat = coef[0] * (up[0] + down[0]) + coef[1] * both + coef[2] * (up[2] - down[2])
    return flat + pltpu.roll(rising, 15, 0) + pltpu.roll(falling, 1, 0)


def plane_shifts(first, second, strip, base):
    lane = lanes()
    right_first, right_second = pltpu.roll(first, 1, 1), pltpu.roll(second, 1, 1)
    left_first, left_second = pltpu.roll(first, 127, 1), pltpu.roll(second, 127, 1)
    before = jnp.where(lane == 0, turn(strip, -(base + 7)), right_first)
    middle_before = jnp.where(lane == 0, right_first, right_second)
    after = jnp.where(lane == 127, turn(strip, 127 - (base + 8)), left_second)
    middle_after = jnp.where(lane == 127, left_second, left_first)
    return (
        (first, middle_after + before, middle_after - before),
        (second, after + middle_before, after - middle_before),
    )


def strip_shifts(strip, edges):
    lane = lanes()
    after, before = pltpu.roll(strip, 127, 1), pltpu.roll(strip, 1, 1)
    for base, first, second in edges:
        after = jnp.where(lane == base + 7, turn(first, base + 7), after)
        before = jnp.where(lane == base + 8, turn(second, base + 9), before)
    return strip, after + before, after - before


def kernel(
    state_ref,
    mask_ref,
    layer_ref,
    fibre_ref,
    out_ref,
    cells,
    packed,
    keep,
    mask,
    strip_cells,
    strip_packed,
    strip_keep,
    strip_mask,
    coef,
    hop_out,
    hop_in,
    first_out,
    first_in,
    gates_out,
    side_out,
    side_in,
    relay_out,
    relay_in,
    relay_gates_out,
    relay_gates_in,
    hop_send,
    hop_recv,
    first_send,
    first_recv,
    gates_send,
    gates_recv,
    side_send,
    side_recv,
    relay_send,
    relay_recv,
    load_sem,
    store_sem,
):
    me_x, me_y = lax.axis_index("gx"), lax.axis_index("gy")
    size_x, size_y = lax.axis_size("gx"), lax.axis_size("gy")
    above = lax.rem(me_x + 1, size_x)
    below = lax.rem(me_x + size_x - 1, size_x)
    right = lax.rem(me_y + 1, size_y)
    left = lax.rem(me_y + size_y - 1, size_y)
    along_x = ((above, me_y), (below, me_y))
    along_y = ((me_x, right), (me_x, left))

    barrier = pltpu.get_barrier_semaphore()
    for target in along_x + along_y:
        pl.semaphore_signal(barrier, inc=1, device_id=target, device_id_type=MESH)

    def remote(source, target, sends, recvs, device):
        return pltpu.make_async_remote_copy(
            src_ref=source,
            dst_ref=target,
            send_sem=sends,
            recv_sem=recvs,
            device_id=device,
            device_id_type=MESH,
        )

    loads = [
        pltpu.make_async_copy(state_ref.at[:, plane], cells.at[:, plane + 1], load_sem.at[plane])
        for plane in range(INNER)
    ]
    for plane in (0, 7, 1, 6, 2, 5, 3, 4):
        loads[plane].start()

    lane = lanes()
    coefficients(layer_ref, fibre_ref, coef)
    spread_tile = jnp.zeros((16, 128), jnp.float32)
    for plane in range(INNER):
        blocks = (mask_ref[plane] > 0).astype(jnp.float32)
        for half in range(2):
            tile = jnp.broadcast_to(blocks[:, half : half + 1], (16, 128))
            mask[plane + 2, :, half * 128 : half * 128 + 128] = tile
            spread_tile = jnp.where(lane == 2 * plane + half, tile, spread_tile)

    def react_plane(slot, parity):
        for top in (0, 8):
            rows = pl.ds(top, 8)
            inside = mask[slot + 1, rows] > 0.0
            fresh = react([cells[comp, slot, rows] for comp in range(COMPS)], inside)
            for comp in range(COMPS):
                cells[comp, slot, rows] = fresh[comp]
            packed[parity, slot + 1, rows] = jnp.where(inside, fresh[0], 0.0)

    def react_strip(which, parity):
        for top in (0, 8):
            rows = pl.ds(top, 8)
            inside = strip_mask[which, rows] > 0.0
            fresh = react([strip_cells[which, comp, rows] for comp in range(COMPS)], inside)
            for comp in range(COMPS):
                strip_cells[which, comp, rows] = fresh[comp]
            strip_packed[parity, which, rows] = jnp.where(inside, fresh[0], 0.0)

    def react_pair(pair, carry, parity):
        react_plane(pair + 1, parity)
        react_plane(8 - pair, parity)
        return carry

    for pair in range(4):
        loads[pair].wait()
        loads[7 - pair].wait()

    lax.fori_loop(0, 4, lambda pair, carry: react_pair(pair, carry, 0), 0)

    for way, (edge, inward) in enumerate(((7, 6), (0, 1))):
        first_out[way, :, 0:256] = packed[0, inward + 2]
        first_out[way, :, 256:512] = cells[0, edge + 1]
        first_out[way, :, 512:640] = spread_tile
        gates_out[way] = cells[1:12, edge + 1]

    def pack_side(read):
        tile = jnp.zeros((16, 128), jnp.float32)
        for plane in range(INNER):
            first, second = read(plane)
            base = plane * 16
            tile = jnp.where((lane >= base) & (lane < base + 8), turn(second, base + 8), tile)
            tile = jnp.where((lane >= base + 8) & (lane < base + 16), turn(first, base + 8), tile)
        return tile

    def own(comp):
        return lambda plane: (cells[comp, plane + 1, :, 0:128], cells[comp, plane + 1, :, 128:256])

    side_out[0] = pack_side(own(0))
    side_out[1] = pack_side(lambda plane: (mask[plane + 2, :, 0:128], mask[plane + 2, :, 128:256]))
    for comp in range(1, COMPS):
        side_out[comp + 1] = pack_side(own(comp))

    pl.semaphore_wait(barrier, 4)
    early, late, lead, bulk, pass_on, pass_gates = [], [], [], [], [], []
    for way in range(2):
        early.append(
            remote(
                side_out.at[pl.ds(0, 2)],
                side_in.at[way, pl.ds(0, 2)],
                side_send.at[0, way],
                side_recv.at[0, way],
                along_y[way],
            )
        )
        lead.append(
            remote(
                first_out.at[way],
                first_in.at[way],
                first_send.at[way],
                first_recv.at[way],
                along_x[way],
            )
        )
        late.append(
            remote(
                side_out.at[pl.ds(2, 11)],
                side_in.at[way, pl.ds(2, 11)],
                side_send.at[1, way],
                side_recv.at[1, way],
                along_y[way],
            )
        )
        bulk.append(
            remote(
                gates_out.at[way],
                cells.at[pl.ds(1, 11), 0 if way == 0 else 9],
                gates_send.at[way],
                gates_recv.at[way],
                along_x[way],
            )
        )
        pass_on.append(
            remote(
                relay_out.at[way],
                relay_in.at[way],
                relay_send.at[0, way],
                relay_recv.at[0, way],
                along_x[way],
            )
        )
        pass_gates.append(
            remote(
                relay_gates_out.at[way],
                relay_gates_in.at[way],
                relay_send.at[1, way],
                relay_recv.at[1, way],
                along_x[way],
            )
        )
    for copies in (early, lead, late, bulk):
        for copy in copies:
            copy.start()

    from_left = lax.rem(lane, 16) < 8
    for copy in early:
        copy.wait_recv()
    strip_cells[0, 0] = jnp.where(from_left, side_in[0, 0], side_in[1, 0])
    reach_left = jnp.where(me_y > 0, 1.0, 0.0)
    reach_right = jnp.where(me_y < size_y - 1, 1.0, 0.0)
    strip_mask[0] = jnp.where(from_left, side_in[0, 1] * reach_left, side_in[1, 1] * reach_right)
    strip_packed[0, 0] = strip_mask[0] * strip_cells[0, 0]
    for way, (edge, inward) in enumerate(((7, 6), (0, 1))):
        tile = jnp.zeros((16, 128), jnp.float32)
        parts = (
            (strip_cells[0, 0], edge),
            (strip_mask[0], edge),
            (strip_mask[0], inward),
            (strip_packed[0, 0], inward),
        )
        for group, (part, plane) in enumerate(parts):
            here = (lane >= group * 16) & (lane < group * 16 + 16)
            tile = jnp.where(here, turn(part, group * 16 - plane * 16), tile)
        relay_out[way] = tile
        pass_on[way].start()

    for copy in late:
        copy.wait_recv()
    for comp in range(1, COMPS):
        strip_cells[0, comp] = jnp.where(from_left, side_in[0, comp + 1], side_in[1, comp + 1])
    for way, edge in enumerate((7, 0)):
        for half, gates in enumerate((range(1, 9), range(9, 12))):
            tile = jnp.zeros((16, 128), jnp.float32)
            for group, comp in enumerate(gates):
                here = (lane >= group * 16) & (lane < group * 16 + 16)
                tile = jnp.where(here, turn(strip_cells[0, comp], group * 16 - edge * 16), tile)
            relay_gates_out[way, :, half * 128 : half * 128 + 128] = tile
        pass_gates[way].start()

    for copy in lead:
        copy.wait_recv()
    for copy in pass_on:
        copy.wait_recv()
    reach = (jnp.where(me_x > 0, 1.0, 0.0), jnp.where(me_x < size_x - 1, 1.0, 0.0))
    outer_mask = jnp.zeros((16, 128), jnp.float32)
    outer_far_mask = jnp.zeros((16, 128), jnp.float32)
    outer_first = jnp.zeros((16, 128), jnp.float32)
    for way, (edge, inward, slot, far) in enumerate(((7, 6, 1, 0), (0, 1, 10, 11))):
        for half in range(2):
            columns = slice(half * 128, half * 128 + 128)
            for plane, target in ((edge, slot), (inward, far)):
                index = 512 + 2 * plane + half
                mask[target, :, columns] = (
                    jnp.broadcast_to(first_in[way, :, index : index + 1], (16, 128)) * reach[way]
                )
        cells[0, slot - 1] = first_in[way, :, 256:512]
        packed[0, slot] = mask[slot] * first_in[way, :, 256:512]
        hop_in[way, 0, :, 0:256] = first_in[way, :, 0:256]
        place = way * 16
        here = (lane >= place) & (lane < place + 16)
        relayed = relay_in[way]
        outer_first = jnp.where(here, turn(relayed, place), outer_first)
        outer_mask = jnp.where(here, turn(relayed, place - 16) * reach[way], outer_mask)
        outer_far_mask = jnp.where(here, turn(relayed, place - 32) * reach[way], outer_far_mask)
        hop_in[way, 0, :, 256:384] = turn(relayed, inward * 16 - 48)
    strip_cells[1, 0] = outer_first
    strip_mask[1] = outer_mask
    strip_packed[0, 1] = outer_mask * outer_first

    def inner_sums(read, strip, outer, planes, emit, emit_strip):
        factors = [coef[index] for index in range(9)]
        shifts, edges = {}, {}
        for plane in range(min(planes) - 1, max(planes) + 2):
            tiles = read(plane)
            if 0 <= plane < INNER:
                shifts[plane] = plane_shifts(*tiles, strip, plane * 16)
            else:
                shifts[plane] = plane_shifts(*tiles, outer, 0 if plane < 0 else 16)
            edges[plane] = tiles
        if emit_strip is not None:
            inner = strip_shifts(strip, [(16 * p, *edges[p]) for p in range(INNER)])
            rim = strip_shifts(outer, [(0, *edges[-1]), (16, *edges[INNER])])
            up = [
                jnp.where(lane >= 112, turn(beyond, 96), turn(part, 112))
                for part, beyond in zip(inner, rim)
            ]
            down = [
                jnp.where(lane < 16, beyond, turn(part, 16)) for part, beyond in zip(inner, rim)
            ]
            emit_strip(tile_sum(factors, inner, up, down))
        for plane in planes:
            for half in range(2):
                total = tile_sum(
                    factors,
                    shifts[plane][half],
                    shifts[plane + 1][half],
                    shifts[plane - 1][half],
                )
                emit(plane, half, total)

    def outer_sums(read, strip, outer, far, emit, emit_strip):
        factors = [coef[index] for index in range(9)]
        rims, insides, fars = [], [], []
        far_tile = jnp.zeros((16, 128), jnp.float32)
        far_edges, rim_edges = [], []
        near_tile = jnp.where(lane < 16, strip, turn(strip, 32))
        near_edges = []
        for way, (rim, near) in enumerate(((-1, 0), (INNER, INNER - 1))):
            rim_tiles, near_tiles = read(rim), read(near)
            first, second, far_strip, base = far(way)
            rims.append(plane_shifts(*rim_tiles, outer, way * 16))
            insides.append(plane_shifts(*near_tiles, strip, near * 16))
            fars.append(plane_shifts(first, second, far_strip, base))
            place = way * 16
            here = (lane >= place) & (lane < place + 16)
            far_tile = jnp.where(here, turn(far_strip, place - base), far_tile)
            far_edges.append((place, first, second))
            rim_edges.append((place, *rim_tiles))
            near_edges.append((place, *near_tiles))
        rim = strip_shifts(outer, rim_edges)
        near = strip_shifts(near_tile, near_edges)
        far_shift = strip_shifts(far_tile, far_edges)
        lower = lane < 16
        up = [jnp.where(lower, a, b) for a, b in zip(near, far_shift)]
        down = [jnp.where(lower, b, a) for a, b in zip(near, far_shift)]
        emit_strip(tile_sum(factors, rim, up, down))
        for way, plane in enumerate((-1, INNER)):
            for half in range(2):
                toward, away = insides[way][half], fars[way][half]
                pair = (toward, away) if way == 0 else (away, toward)
                emit(plane, half, tile_sum(factors, rims[way][half], *pair))

    def mask_tiles(plane):
        return mask[plane + 2, :, 0:128], mask[plane + 2, :, 128:256]

    def keep_plane(plane, half, total):
        columns = slice(half * 128, half * 128 + 128)
        keep[plane + 1, :, columns] = 1.0 - mask[plane + 2, :, columns] * total

    def keep_strip(which):
        def emit(total):
            strip_keep[which] = 1.0 - strip_mask[which] * total

        return emit

    inner_sums(
        mask_tiles, strip_mask[0], strip_mask[1], range(INNER), keep_plane, keep_strip(0)
    )
    outer_sums(
        mask_tiles,
        strip_mask[0],
        strip_mask[1],
        lambda way: (*mask_tiles(-2 if way == 0 else 9), outer_far_mask, way * 16),
        keep_plane,
        keep_strip(1),
    )

    def move_plane(plane, half, total):
        columns = slice(half * 128, half * 128 + 128)
        cells[0, plane + 1, :, columns] = (
            cells[0, plane + 1, :, columns] * keep[plane + 1, :, columns]
            + mask[plane + 2, :, columns] * total
        )

    def move_strip(which):
        def emit(total):
            strip_cells[which, 0] = (
                strip_cells[which, 0] * strip_keep[which] + strip_mask[which] * total
            )

        return emit

    def packed_tiles(parity):
        return lambda plane: (
            packed[parity, plane + 2, :, 0:128],
            packed[parity, plane + 2, :, 128:256],
        )

    def hop(way, step):
        return remote(
            hop_out.at[way, lax.rem(step, 2)],
            hop_in.at[way, step],
            hop_send.at[way, step],
            hop_recv.at[way, step],
            along_x[way],
        )

    def advance(step, carry):
        now = lax.rem(step, 2)
        old = 1 - now
        inner_sums(
            packed_tiles(old),
            strip_packed[old, 0],
            strip_packed[old, 1],
            range(INNER),
            move_plane,
            move_strip(0),
        )
        react_strip(0, now)
        react_pair(1, 0, now)

        @pl.when(step < HOPS)
        def _():
            @pl.when(step > 2)
            def _():
                for way in range(2):
                    hop(way, step - 2).wait_send()

            for way, inward in enumerate((6, 1)):
                hop_out[way, now, :, 0:256] = packed[now, inward + 2]
                hop_out[way, now, :, 256:384] = strip_packed[now, 0]
                hop(way, step).start()

        lax.fori_loop(2, 4, lambda pair, kept: react_pair(pair, kept, now), 0)
        react_pair(0, 0, now)

        @pl.when(step == 1)
        def _():
            for copy in bulk:
                copy.wait_recv()
            for copy in pass_gates:
                copy.wait_recv()
            for half, gates in enumerate((range(1, 9), range(9, 12))):
                for group, comp in enumerate(gates):
                    tile = jnp.zeros((16, 128), jnp.float32)
                    for way in range(2):
                        place = way * 16
                        here = (lane >= place) & (lane < place + 16)
                        source = relay_gates_in[way, :, half * 128 : half * 128 + 128]
                        tile = jnp.where(here, turn(source, place - group * 16), tile)
                    strip_cells[1, comp] = tile

        @pl.when(step > 1)
        def _():
            for way in range(2):
                hop(way, step - 1).wait_recv()

        outer_sums(
            packed_tiles(old),
            strip_packed[old, 0],
            strip_packed[old, 1],
            lambda way: (
                hop_in[way, step - 1, :, 0:128],
                hop_in[way, step - 1, :, 128:256],
                hop_in[way, step - 1, :, 256:384],
                96 if way == 0 else 16,
            ),
            move_plane,
            move_strip(1),
        )
        react_strip(1, now)
        react_plane(0, now)
        react_plane(9, now)
        return carry

    lax.fori_loop(1, STEPS, advance, 0)

    stores = [
        pltpu.make_async_copy(
            cells.at[pl.ds(1, 11), pl.ds(1, INNER)], out_ref.at[pl.ds(1, 11)], store_sem.at[0]
        ),
        pltpu.make_async_copy(cells.at[0, pl.ds(1, INNER)], out_ref.at[0], store_sem.at[1]),
    ]
    stores[0].start()
    last = (STEPS - 1) % 2
    inner_sums(
        packed_tiles(last),
        strip_packed[last, 0],
        strip_packed[last, 1],
        range(INNER),
        move_plane,
        None,
    )
    stores[1].start()
    for copies in (early, lead, late, bulk, pass_on, pass_gates):
        for copy in copies:
            copy.wait_send()
    for way in range(2):
        for step in (HOPS - 2, HOPS - 1):
            hop(way, step).wait_send()
    for copy in stores:
        copy.wait()


def shards(state, tissue_mask, layer_index, fibre):
    vmem, sems = pltpu.VMEM, pltpu.SemaphoreType.DMA
    f32 = jnp.float32
    return pl.pallas_call(
        kernel,
        out_shape=jax.ShapeDtypeStruct(state.shape, f32),
        in_specs=[
            pl.BlockSpec(memory_space=pl.ANY),
            pl.BlockSpec(memory_space=pltpu.VMEM),
            pl.BlockSpec(memory_space=pltpu.SMEM),
            pl.BlockSpec(memory_space=pltpu.SMEM),
        ],
        out_specs=pl.BlockSpec(memory_space=pl.ANY),
        scratch_shapes=[
            vmem((COMPS, 10, 16, 256), f32),
            vmem((2, 12, 16, 256), f32),
            vmem((10, 16, 256), f32),
            vmem((12, 16, 256), f32),
            vmem((2, COMPS, 16, 128), f32),
            vmem((2, 2, 16, 128), f32),
            vmem((2, 16, 128), f32),
            vmem((2, 16, 128), f32),
            vmem((9, 16, 128), f32),
            vmem((2, 2, 16, 384), f32),
            vmem((2, HOPS, 16, 384), f32),
            vmem((2, 16, 640), f32),
            vmem((2, 16, 640), f32),
            vmem((2, 11, 16, 256), f32),
            vmem((13, 16, 128), f32),
            vmem((2, 13, 16, 128), f32),
            vmem((2, 16, 128), f32),
            vmem((2, 16, 128), f32),
            vmem((2, 16, 256), f32),
            vmem((2, 16, 256), f32),
            sems((2, HOPS)),
            sems((2, HOPS)),
            sems((2,)),
            sems((2,)),
            sems((2,)),
            sems((2,)),
            sems((2, 2)),
            sems((2, 2)),
            sems((2, 2)),
            sems((2, 2)),
            sems((INNER,)),
            sems((2,)),
        ],
        compiler_params=pltpu.CompilerParams(collective_id=0, has_side_effects=True),
        name="slab",
    )(state, tissue_mask, layer_index, fibre)


def solution(mesh):
    placed = (P(None, "gx", None, "gy"), P("gx", None, "gy"), P(), P())
    return jax.shard_map(
        shards, mesh=mesh, in_specs=placed, out_specs=P(None, "gx", None, "gy"), check_vma=False
    )
```

```python
import math

import jax
import jax.numpy as jnp
from jax import lax
from jax.experimental import pallas as pl
from jax.experimental.pallas import tpu as pltpu
from jax.sharding import PartitionSpec as P

STEPS = 8
TRANSVERSE = 0.04
LONGITUDINAL = 0.12
DT = 0.02
RTF = 8314.472 * 310.0 / 96485.3415
EK = RTF * math.log(5.4 / 138.3)
ENA = RTF * math.log(140.0 / 7.67)
EKS = RTF * math.log((5.4 + 0.03 * 140.0) / (138.3 + 0.03 * 7.67))
L2E = 1.0 / math.log(2.0)
KAPPA = -DT * L2E


def grow(volt, slope):
    return jnp.exp2(volt * (slope * L2E))


def sig(volt, centre, width):
    return jax.nn.sigmoid(volt * (1.0 / width) + (-centre / width))


def settle(gate, steady, factor):
    return steady + (gate - steady) * jnp.exp2(factor)


def membrane(s):
    x, m, h, j, d, f, r, z, p, q, w, ca = s
    v = x * 100.0
    over = v - EK
    b = grow(v, 0.05)
    ib = 1.0 / b
    b2 = b * b
    ib2 = ib * ib
    c = jnp.maximum(ca, 0.02)
    vca = (v - 0.5 * RTF * math.log(2000.0)) + (0.5 * RTF) * jnp.log(c)
    sodium = ((14.838 * m) * (m * m) * (h * j) + 0.00029) * (v - ENA)
    calcium = (0.08 * d * f + 0.000592) * vca
    sa = sig(v, EK + 200.0, -1.0 / 0.06)
    bk = (
        (30.0 * math.exp(0.0002 * (100.0 - EK))) * grow(v, 0.0002)
        + (10.0 * math.exp(0.1 * (-EK - 10.0))) * b2
    ) * sig(v, EK, 2.0)
    inward = 5.405 * sa / (sa + bk)
    potassium = (
        0.294 * r * z + 0.153 * p * q + inward + 0.0146 * sig(v, 25.0, 5.98)
    ) * over
    slow = (0.392 * w) * w * (v - EKS)
    en = grow(v, -1.0 / RTF)
    pump = (2.724 * 5.4 / 6.4 * 7.67 / 47.67) / (
        1.0 + 0.1245 * grow(v, -0.1 / RTF) + 0.0353 * en
    )
    ef = grow(v, 0.35 / RTF)
    eg = ef * en
    scale = 1000.0 / ((87.5**3 + 140.0**3) * 3.38)
    exchange = (
        (scale * 7.67**3 * 2.0) * ef - (scale * 2.5 * 140.0**3 * 0.001) * eg * c
    ) / (1.0 + 0.1 * eg)
    pump_ca = 0.1238 * c / (c + 0.5)
    total = sodium + calcium + potassium + slow + pump + exchange + pump_ca
    nx = x - (DT / 100.0) * total
    nca = ca - (DT * 0.05) * (calcium + pump_ca - 2.0 * exchange)
    low = 1.0 / (1.0 + math.exp(20.0) * grow(v, 0.5))
    nm = settle(
        m,
        sig(v, -56.86, 9.03) ** 2,
        (10.0 * KAPPA + (10.0 * KAPPA * math.exp(-12.0)) * (ib2 * ib2))
        / (sig(v, -35.0, -5.0) + sig(v, 50.0, -200.0)),
    )
    hs = sig(v, -71.55, -7.43)
    hs = hs * hs
    up = (KAPPA * 0.77 / 0.13) * sig(v, -10.66, 11.1)
    dn = (
        (KAPPA * 0.057 * math.exp(-80.0 / 6.8)) * grow(v, -1.0 / 6.8)
        + (KAPPA * 2.7) * grow(v, 0.079)
        + (KAPPA * 310000.0) * grow(v, 0.3485)
    )
    nh = settle(h, hs, up + low * (dn - up))
    up = (KAPPA * 0.6) * grow(v, 0.057) * sig(v, -32.0, 10.0)
    dn = ((KAPPA * -25428.0) * grow(v, 0.2444) - (KAPPA * 6.948e-06) * grow(v, -0.04391)) * (
        v + 37.78
    ) * sig(v, -79.23, -1.0 / 0.311) + (KAPPA * 0.02424) * grow(v, -0.01052) * sig(
        v, -40.14, 1.0 / 0.1378
    )
    nj = settle(j, hs, up + low * (dn - up))
    nd = settle(
        d,
        sig(v, -8.0, 7.5),
        KAPPA
        / ((1.96 * sig(v, -35.0, 13.0) + 0.35) * sig(v, -5.0, -5.0) + sig(v, 50.0, 20.0)),
    )
    t = v + 27.0
    nf = settle(
        f,
        sig(v, -20.0, -7.0),
        1.0
        / (
            (1102.5 / KAPPA) * jnp.exp2(t * t * (-L2E / 225.0))
            + (200.0 / KAPPA) * sig(v, 13.0, 10.0)
            + (180.0 / KAPPA) * sig(v, -30.0, -10.0)
            + 20.0 / KAPPA
        ),
    )
    t = v + 40.0
    nr = settle(
        r,
        sig(v, 20.0, 6.0),
        1.0 / ((9.5 / KAPPA) * jnp.exp2(t * t * (-L2E / 1800.0)) + 0.8 / KAPPA),
    )
    t = v + 45.0
    nz = settle(
        z,
        sig(v, -20.0, -5.0),
        1.0
        / (
            (85.0 / KAPPA) * jnp.exp2(t * t * (-L2E / 320.0))
            + (5.0 / KAPPA) * sig(v, 20.0, -5.0)
            + 3.0 / KAPPA
        ),
    )
    k = KAPPA / 2700.0
    np_ = settle(
        p,
        sig(v, -26.0, 7.0),
        (k + (k * math.exp(-4.5)) * ib2)
        * (1.0 + math.exp(30.0 / 11.5) * grow(v, 1.0 / 11.5)),
    )
    k = KAPPA / 3.36
    nq = settle(
        q,
        sig(v, -88.0, -24.0),
        (k * (1.0 + math.exp(-6.0))) + (k * math.exp(-3.0)) * (b + ib),
    )
    nw = settle(
        w,
        sig(v, -5.0, 14.0),
        1.0
        / (
            lax.rsqrt(1.0 + math.exp(5.0 / 6.0) * grow(v, -1.0 / 6.0))
            * ((1400.0 / KAPPA) * sig(v, 35.0, -15.0))
            + 80.0 / KAPPA
        ),
    )
    return nx, nm, nh, nj, nd, nf, nr, nz, np_, nq, nw, nca


INNER = 8
COMPS = 12
HOPS = STEPS - 1
MESH = pl.DeviceIdType.MESH


def react(state, inside):
    fresh = membrane(state)
    return [jnp.where(inside, new, old) for new, old in zip(fresh, state)]


def lanes():
    return lax.broadcasted_iota(jnp.int32, (16, 128), 1)


def turn(tile, shift):
    shift = shift % 128
    return tile if shift == 0 else pltpu.roll(tile, shift, 1)


def coefficients(layer_ref, fibre_ref, coef):
    row = lax.broadcasted_iota(jnp.int32, (16, 128), 0)
    angle_in = jnp.zeros((16, 128), jnp.float32)
    angle_out = jnp.zeros((16, 128), jnp.float32)
    for level in range(16):
        layer = layer_ref[level]
        angle_in = jnp.where(row == level, fibre_ref[0, layer], angle_in)
        angle_out = jnp.where(row == level, fibre_ref[1, layer], angle_out)
    along_x = jnp.cos(angle_in) * jnp.cos(angle_out)
    along_y = jnp.sin(angle_in) * jnp.cos(angle_out)
    along_z = jnp.sin(angle_out)
    spread = LONGITUDINAL - TRANSVERSE
    coef[0] = TRANSVERSE + spread * along_x * along_x
    coef[1] = TRANSVERSE + spread * along_y * along_y
    coef[2] = spread * along_x * along_y / 2.0
    parts = (
        TRANSVERSE + spread * along_z * along_z,
        spread * along_x * along_z / 2.0,
        spread * along_y * along_z / 2.0,
    )
    for index, part in enumerate(parts):
        below = (part + pltpu.roll(part, 1, 0)) / 2.0
        above = (part + pltpu.roll(part, 15, 0)) / 2.0
        coef[3 + index] = jnp.where(row == 0, 0.0, below)
        coef[6 + index] = jnp.where(row == 15, 0.0, above)


def tile_sum(coef, here, up, down):
    value, both, slope = here
    across = up[0] - down[0]
    rising = coef[3] * value + coef[4] * across + coef[5] * slope
    falling = coef[6] * value - coef[7] * across - coef[8] * slope
    flat = coef[0] * (up[0] + down[0]) + coef[1] * both + coef[2] * (up[2] - down[2])
    return flat + pltpu.roll(rising, 15, 0) + pltpu.roll(falling, 1, 0)


def plane_shifts(first, second, strip, base):
    lane = lanes()
    right_first, right_second = pltpu.roll(first, 1, 1), pltpu.roll(second, 1, 1)
    left_first, left_second = pltpu.roll(first, 127, 1), pltpu.roll(second, 127, 1)
    before = jnp.where(lane == 0, turn(strip, -(base + 7)), right_first)
    middle_before = jnp.where(lane == 0, right_first, right_second)
    after = jnp.where(lane == 127, turn(strip, 127 - (base + 8)), left_second)
    middle_after = jnp.where(lane == 127, left_second, left_first)
    return (
        (first, middle_after + before, middle_after - before),
        (second, after + middle_before, after - middle_before),
    )


def strip_shifts(strip, edges):
    lane = lanes()
    after, before = pltpu.roll(strip, 127, 1), pltpu.roll(strip, 1, 1)
    for base, first, second in edges:
        after = jnp.where(lane == base + 7, turn(first, base + 7), after)
        before = jnp.where(lane == base + 8, turn(second, base + 9), before)
    return strip, after + before, after - before


def kernel(
    state_ref,
    mask_ref,
    layer_ref,
    fibre_ref,
    out_ref,
    cells,
    packed,
    keep,
    mask,
    strip_cells,
    strip_packed,
    strip_keep,
    strip_mask,
    far_mask,
    coef,
    hop_in,
    hop_strip_in,
    spread_out,
    spread_in,
    side_out,
    side_in,
    relay_out,
    relay_in,
    relay_gates_out,
    relay_gates_in,
    hop_send,
    hop_recv,
    strip_send,
    strip_recv,
    lead_send,
    lead_recv,
    side_send,
    side_recv,
    relay_send,
    relay_recv,
    load_sem,
    store_sem,
):
    me_x, me_y = lax.axis_index("gx"), lax.axis_index("gy")
    size_x, size_y = lax.axis_size("gx"), lax.axis_size("gy")
    along_x = ((me_x + 1, me_y), (me_x - 1, me_y))
    along_y = ((me_x, me_y + 1), (me_x, me_y - 1))
    ends_x = (me_x < size_x - 1, me_x > 0)
    ends_y = (me_y < size_y - 1, me_y > 0)
    ways = (0, 1)

    def sending(ends, way, action):
        pl.when(ends[way])(action)

    def receiving(ends, way, action):
        pl.when(ends[1 - way])(action)

    barrier = pltpu.get_barrier_semaphore()
    for ends, targets in ((ends_x, along_x), (ends_y, along_y)):
        for way in ways:

            def greet(target=targets[way]):
                pl.semaphore_signal(barrier, inc=1, device_id=target, device_id_type=MESH)

            sending(ends, way, greet)

    def remote(source, target, sends, recvs, device):
        return pltpu.make_async_remote_copy(
            src_ref=source,
            dst_ref=target,
            send_sem=sends,
            recv_sem=recvs,
            device_id=device,
            device_id_type=MESH,
        )

    loads = [
        pltpu.make_async_copy(state_ref.at[:, plane], cells.at[:, plane + 1], load_sem.at[plane])
        for plane in range(INNER)
    ]
    for plane in (0, 7, 1, 6, 2, 5, 3, 4):
        loads[plane].start()

    lane = lanes()
    coefficients(layer_ref, fibre_ref, coef)
    spread_tile = jnp.zeros((16, 128), jnp.float32)
    unit = (
        lax.broadcasted_iota(jnp.int32, (16, 16), 0) == lax.broadcasted_iota(jnp.int32, (16, 16), 1)
    ).astype(jnp.float32)
    for plane in range(INNER):
        blocks = lax.dot_general(
            unit,
            (mask_ref[plane] > 0).astype(jnp.float32),
            (((1,), (1,)), ((), ())),
            preferred_element_type=jnp.float32,
        )
        for half in range(2):
            tile = jnp.broadcast_to(blocks[:, half : half + 1], (16, 128))
            mask[plane + 2, :, half * 128 : half * 128 + 128] = tile
            spread_tile = jnp.where(lane == 2 * plane + half, tile, spread_tile)
    spread_out[...] = spread_tile

    for way in ways:

        @pl.when(jnp.logical_not(ends_x[1 - way]))
        def _(way=way):
            for step in range(HOPS):
                hop_in[way, step] = jnp.zeros((16, 256), jnp.float32)
                hop_strip_in[way, step] = jnp.zeros((16, 128), jnp.float32)
            spread_in[way] = jnp.zeros((16, 128), jnp.float32)
            relay_in[way] = jnp.zeros((16, 128), jnp.float32)
            relay_gates_in[way] = jnp.zeros((16, 256), jnp.float32)
            for comp in range(COMPS):
                cells[comp, 0 if way == 0 else 9] = jnp.zeros((16, 256), jnp.float32)

        @pl.when(jnp.logical_not(ends_y[1 - way]))
        def _(way=way):
            for comp in range(COMPS + 1):
                side_in[way, comp] = jnp.zeros((16, 128), jnp.float32)

    def react_plane(slot, parity):
        for top in (0, 8):
            rows = pl.ds(top, 8)
            inside = mask[slot + 1, rows] > 0.0
            fresh = react([cells[comp, slot, rows] for comp in range(COMPS)], inside)
            for comp in range(COMPS):
                cells[comp, slot, rows] = fresh[comp]
            packed[parity, slot + 1, rows] = jnp.where(inside, fresh[0], 0.0)

    def react_strip(which, parity):
        for top in (0, 8):
            rows = pl.ds(top, 8)
            inside = strip_mask[which, rows] > 0.0
            fresh = react([strip_cells[which, comp, rows] for comp in range(COMPS)], inside)
            for comp in range(COMPS):
                strip_cells[which, comp, rows] = fresh[comp]
            strip_packed[parity, which, rows] = jnp.where(inside, fresh[0], 0.0)

    def react_pair(pair, parity):
        react_plane(pair + 1, parity)
        react_plane(8 - pair, parity)

    for copy in loads:
        copy.wait()

    def first_pair(pair, carry):
        react_pair(pair, 0)
        return carry

    lax.fori_loop(0, 4, first_pair, 0)

    def pack_side(read):
        tile = jnp.zeros((16, 128), jnp.float32)
        for plane in range(INNER):
            first, second = read(plane)
            base = plane * 16
            tile = jnp.where((lane >= base) & (lane < base + 8), turn(second, base + 8), tile)
            tile = jnp.where((lane >= base + 8) & (lane < base + 16), turn(first, base + 8), tile)
        return tile

    def own(comp):
        return lambda plane: (cells[comp, plane + 1, :, 0:128], cells[comp, plane + 1, :, 128:256])

    side_out[0] = pack_side(own(0))
    side_out[1] = pack_side(lambda plane: (mask[plane + 2, :, 0:128], mask[plane + 2, :, 128:256]))
    for comp in range(1, COMPS):
        side_out[comp + 1] = pack_side(own(comp))

    peers = sum(end.astype(jnp.int32) for end in ends_x + ends_y)
    pl.semaphore_wait(barrier, peers)

    early, late, lead, bulk, relay, relay_gates = [], [], [], [], [], []
    for way, (edge, inward, slot) in enumerate(((7, 6, 0), (0, 1, 9))):
        early.append(
            remote(
                side_out.at[pl.ds(0, 2)],
                side_in.at[way, pl.ds(0, 2)],
                side_send.at[0, way],
                side_recv.at[0, way],
                along_y[way],
            )
        )
        late.append(
            remote(
                side_out.at[pl.ds(2, 11)],
                side_in.at[way, pl.ds(2, 11)],
                side_send.at[1, way],
                side_recv.at[1, way],
                along_y[way],
            )
        )
        lead.append(
            [
                remote(
                    source, target, lead_send.at[index, way], lead_recv.at[index, way], along_x[way]
                )
                for index, (source, target) in enumerate(
                    (
                        (cells.at[0, edge + 1], cells.at[0, slot]),
                        (packed.at[0, inward + 2], hop_in.at[way, 0]),
                        (spread_out, spread_in.at[way]),
                    )
                )
            ]
        )
        bulk.append(
            [
                remote(
                    cells.at[pl.ds(start, size), edge + 1],
                    cells.at[pl.ds(start, size), slot],
                    lead_send.at[index, way],
                    lead_recv.at[index, way],
                    along_x[way],
                )
                for index, start, size in ((3, 1, 5), (4, 6, 6))
            ]
        )
        relay.append(
            remote(
                relay_out.at[way],
                relay_in.at[way],
                relay_send.at[0, way],
                relay_recv.at[0, way],
                along_x[way],
            )
        )
        relay_gates.append(
            remote(
                relay_gates_out.at[way],
                relay_gates_in.at[way],
                relay_send.at[1, way],
                relay_recv.at[1, way],
                along_x[way],
            )
        )
    for way in ways:
        sending(ends_y, way, early[way].start)
    for way in ways:
        for copy in lead[way]:
            sending(ends_x, way, copy.start)
    for way in ways:
        sending(ends_y, way, late[way].start)
        sending(ends_x, way, bulk[way][0].start)

    from_left = lax.rem(lane, 16) < 8
    for way in ways:
        receiving(ends_y, way, early[way].wait_recv)
    strip_cells[0, 0] = jnp.where(from_left, side_in[0, 0], side_in[1, 0])
    strip_mask[0] = jnp.where(from_left, side_in[0, 1], side_in[1, 1])
    strip_packed[0, 0] = strip_mask[0] * strip_cells[0, 0]
    for way, (edge, inward) in enumerate(((7, 6), (0, 1))):
        tile = jnp.zeros((16, 128), jnp.float32)
        parts = (
            (strip_cells[0, 0], edge),
            (strip_mask[0], edge),
            (strip_mask[0], inward),
            (strip_packed[0, 0], inward),
        )
        for group, (part, plane) in enumerate(parts):
            here = (lane >= group * 16) & (lane < group * 16 + 16)
            tile = jnp.where(here, turn(part, group * 16 - plane * 16), tile)
        relay_out[way] = tile
        sending(ends_x, way, relay[way].start)
        sending(ends_x, way, bulk[way][1].start)

    def base_of(plane):
        return (0, plane * 16) if 0 <= plane < INNER else (1, 0 if plane < 0 else 16)

    def shift_planes(read, strips, planes):
        shifts = {}
        for plane in planes:
            which, base = base_of(plane)
            shifts[plane] = plane_shifts(*read(plane), strips[which], base)
        return shifts

    def emit_planes(factors, shifts, planes, emit):
        for plane in planes:
            for half in range(2):
                total = tile_sum(
                    factors,
                    shifts[plane][half],
                    shifts[plane + 1][half],
                    shifts[plane - 1][half],
                )
                emit(plane, half, total)

    def load_factors():
        return [coef[index] for index in range(9)]

    def inner_sums(read, strips, emit):
        shifts = shift_planes(read, strips, range(INNER))
        emit_planes(load_factors(), shifts, range(1, INNER - 1), emit)

    def strip_sums(read, strips, emit_strip):
        inner = strip_shifts(strips[0], [(16 * p, *read(p)) for p in range(INNER)])
        rim = strip_shifts(strips[1], [(0, *read(-1)), (16, *read(INNER))])
        up = [
            jnp.where(lane >= 112, turn(beyond, 96), turn(part, 112))
            for part, beyond in zip(inner, rim)
        ]
        down = [jnp.where(lane < 16, beyond, turn(part, 16)) for part, beyond in zip(inner, rim)]
        emit_strip(tile_sum(load_factors(), inner, up, down))

    def edge_sums(read, strips, emit):
        shifts = shift_planes(read, strips, (-1, 0, 1, 6, 7, 8))
        emit_planes(load_factors(), shifts, (0, 7), emit)

    def rim_strip_sums(read, strips, far, emit_strip):
        far_tile = jnp.zeros((16, 128), jnp.float32)
        far_edges, rim_edges, near_edges = [], [], []
        for way, (rim, near) in enumerate(((-1, 0), (INNER, INNER - 1))):
            first, second, far_strip, base = far(way)
            place = way * 16
            here = (lane >= place) & (lane < place + 16)
            far_tile = jnp.where(here, turn(far_strip, place - base), far_tile)
            far_edges.append((place, first, second))
            rim_edges.append((place, *read(rim)))
            near_edges.append((place, *read(near)))
        near_tile = jnp.where(lane < 16, strips[0], turn(strips[0], 32))
        rim = strip_shifts(strips[1], rim_edges)
        near = strip_shifts(near_tile, near_edges)
        beyond = strip_shifts(far_tile, far_edges)
        lower = lane < 16
        up = [jnp.where(lower, a, b) for a, b in zip(near, beyond)]
        down = [jnp.where(lower, b, a) for a, b in zip(near, beyond)]
        emit_strip(tile_sum(load_factors(), rim, up, down))

    def rim_sums(read, strips, far, emit):
        shifts = shift_planes(read, strips, (-1, 0, 7, 8))
        shifts[-2] = plane_shifts(*far(0))
        shifts[9] = plane_shifts(*far(1))
        emit_planes(load_factors(), shifts, (-1, INNER), emit)

    def mask_tiles(plane):
        return mask[plane + 2, :, 0:128], mask[plane + 2, :, 128:256]

    def keep_plane(plane, half, total):
        columns = slice(half * 128, half * 128 + 128)
        keep[plane + 1, :, columns] = 1.0 - mask[plane + 2, :, columns] * total

    def keep_strip(which):
        def emit(total):
            strip_keep[which] = 1.0 - strip_mask[which] * total

        return emit

    def mask_far(way):
        return (*mask_tiles(-2 if way == 0 else 9), far_mask[...], way * 16)

    def move_plane(plane, half, total):
        columns = slice(half * 128, half * 128 + 128)
        cells[0, plane + 1, :, columns] = (
            cells[0, plane + 1, :, columns] * keep[plane + 1, :, columns]
            + mask[plane + 2, :, columns] * total
        )

    def move_strip(which):
        def emit(total):
            strip_cells[which, 0] = (
                strip_cells[which, 0] * strip_keep[which] + strip_mask[which] * total
            )

        return emit

    def tiles(parity):
        return lambda plane: (
            packed[parity, plane + 2, :, 0:128],
            packed[parity, plane + 2, :, 128:256],
        )

    def strips_of(parity):
        return strip_packed[parity, 0], strip_packed[parity, 1]

    def hop(way, step, parity):
        return remote(
            packed.at[parity, 8 if way == 0 else 3],
            hop_in.at[way, step],
            hop_send.at[way, step],
            hop_recv.at[way, step],
            along_x[way],
        )

    def strip_hop(way, step, parity):
        return remote(
            strip_packed.at[parity, 0],
            hop_strip_in.at[way, step],
            strip_send.at[way, step],
            strip_recv.at[way, step],
            along_x[way],
        )

    def rim_step(step, parity):
        def far(way):
            return (
                hop_in[way, step - 1, :, 0:128],
                hop_in[way, step - 1, :, 128:256],
                hop_strip_in[way, step - 1],
                96 if way == 0 else 16,
            )

        read, strips = tiles(parity), strips_of(parity)
        rim_strip_sums(read, strips, far, move_strip(1))
        rim_sums(read, strips, far, move_plane)
        react_strip(1, 1 - parity)

    def rim_planes(parity):
        react_plane(0, parity)
        react_plane(9, parity)

    def open_rim():
        for way in ways:
            for copy in lead[way]:
                receiving(ends_x, way, copy.wait_recv)
            receiving(ends_x, way, relay[way].wait_recv)
        outer_mask = jnp.zeros((16, 128), jnp.float32)
        outer_far_mask = jnp.zeros((16, 128), jnp.float32)
        outer_first = jnp.zeros((16, 128), jnp.float32)
        for way, (edge, inward, slot, beyond) in enumerate(((7, 6, 1, 0), (0, 1, 10, 11))):
            for half in range(2):
                columns = slice(half * 128, half * 128 + 128)
                for plane, target in ((edge, slot), (inward, beyond)):
                    index = 2 * plane + half
                    mask[target, :, columns] = jnp.broadcast_to(
                        spread_in[way, :, index : index + 1], (16, 128)
                    )
            packed[0, slot] = mask[slot] * cells[0, slot - 1]
            place = way * 16
            here = (lane >= place) & (lane < place + 16)
            relayed = relay_in[way]
            outer_first = jnp.where(here, turn(relayed, place), outer_first)
            outer_mask = jnp.where(here, turn(relayed, place - 16), outer_mask)
            outer_far_mask = jnp.where(here, turn(relayed, place - 32), outer_far_mask)
            hop_strip_in[way, 0] = turn(relayed, inward * 16 - 48)
        strip_cells[1, 0] = outer_first
        strip_mask[1] = outer_mask
        strip_packed[0, 1] = outer_mask * outer_first
        far_mask[...] = outer_far_mask
        masks = (strip_mask[0], outer_mask)
        strip_sums(mask_tiles, masks, keep_strip(0))
        edge_sums(mask_tiles, masks, keep_plane)
        rim_strip_sums(mask_tiles, masks, mask_far, keep_strip(1))
        rim_sums(mask_tiles, masks, mask_far, keep_plane)

    def open_rim_gates():
        for way in ways:
            for copy in bulk[way]:
                receiving(ends_x, way, copy.wait_recv)
            receiving(ends_x, way, relay_gates[way].wait_recv)
        for half, gates in enumerate((range(1, 9), range(9, 12))):
            for group, comp in enumerate(gates):
                tile = jnp.zeros((16, 128), jnp.float32)
                for way in ways:
                    place = way * 16
                    here = (lane >= place) & (lane < place + 16)
                    source = relay_gates_in[way, :, half * 128 : half * 128 + 128]
                    tile = jnp.where(here, turn(source, place - group * 16), tile)
                strip_cells[1, comp] = tile

    def open_strip_gates():
        for way in ways:
            receiving(ends_y, way, late[way].wait_recv)
        for comp in range(1, COMPS):
            strip_cells[0, comp] = jnp.where(from_left, side_in[0, comp + 1], side_in[1, comp + 1])
        for way, edge in enumerate((7, 0)):
            for half, gates in enumerate((range(1, 9), range(9, 12))):
                tile = jnp.zeros((16, 128), jnp.float32)
                for group, comp in enumerate(gates):
                    here = (lane >= group * 16) & (lane < group * 16 + 16)
                    tile = jnp.where(here, turn(strip_cells[0, comp], group * 16 - edge * 16), tile)
                relay_gates_out[way, :, half * 128 : half * 128 + 128] = tile
            sending(ends_x, way, relay_gates[way].start)

    inner_sums(mask_tiles, (strip_mask[0], None), keep_plane)

    def advance(step, carry):
        now = lax.rem(step, 2)
        old = 1 - now

        @pl.when(step > 2)
        def _():
            for way in ways:
                sending(ends_x, way, hop(way, step - 2, now).wait_send)

        inner_sums(tiles(old), strips_of(old), move_plane)
        react_pair(1, now)

        @pl.when(step < HOPS)
        def _():
            for way in ways:
                sending(ends_x, way, hop(way, step, now).start)

        def pairs(pair, kept):
            react_pair(pair, now)
            return kept

        lax.fori_loop(2, 4, pairs, 0)

        @pl.when(step == 1)
        def _():
            open_strip_gates()
            open_rim()
            for way in ways:
                for copy in lead[way] + bulk[way]:
                    sending(ends_x, way, copy.wait_send)

        @pl.when(step == 2)
        def _():
            open_rim_gates()

        @pl.when(step > 2)
        def _():
            for way in ways:
                for copy in (hop(way, step - 2, now), strip_hop(way, step - 2, now)):
                    receiving(ends_x, way, copy.wait_recv)
                sending(ends_x, way, strip_hop(way, step - 2, now).wait_send)

        @pl.when(step > 1)
        def _():
            rim_step(step - 1, now)
            rim_planes(old)

        strip_sums(tiles(old), strips_of(old), move_strip(0))
        react_strip(0, now)

        @pl.when(step < HOPS)
        def _():
            for way in ways:
                sending(ends_x, way, strip_hop(way, step, now).start)

        edge_sums(tiles(old), strips_of(old), move_plane)
        react_pair(0, now)
        return carry

    lax.fori_loop(1, STEPS, advance, 0)

    stores = [
        pltpu.make_async_copy(
            cells.at[pl.ds(1, 11), pl.ds(1, INNER)], out_ref.at[pl.ds(1, 11)], store_sem.at[0]
        ),
        pltpu.make_async_copy(cells.at[0, pl.ds(1, INNER)], out_ref.at[0], store_sem.at[1]),
    ]
    stores[0].start()
    last = (STEPS - 1) % 2
    inner_sums(tiles(last), strips_of(last), move_plane)
    for way in ways:
        for copy in (hop(way, HOPS - 1, 1 - last), strip_hop(way, HOPS - 1, 1 - last)):
            receiving(ends_x, way, copy.wait_recv)
    rim_step(STEPS - 1, 1 - last)
    rim_planes(last)
    edge_sums(tiles(last), strips_of(last), move_plane)
    stores[1].start()
    for way in ways:
        for copy in (hop(way, HOPS - 1, 1 - last), strip_hop(way, HOPS - 1, 1 - last)):
            sending(ends_x, way, copy.wait_send)
        sending(ends_y, way, early[way].wait_send)
        sending(ends_y, way, late[way].wait_send)
        sending(ends_x, way, relay[way].wait_send)
        sending(ends_x, way, relay_gates[way].wait_send)
    for copy in stores:
        copy.wait()


def shards(state, tissue_mask, layer_index, fibre):
    vmem, sems = pltpu.VMEM, pltpu.SemaphoreType.DMA
    f32 = jnp.float32
    return pl.pallas_call(
        kernel,
        out_shape=jax.ShapeDtypeStruct(state.shape, f32),
        in_specs=[
            pl.BlockSpec(memory_space=pl.ANY),
            pl.BlockSpec(memory_space=pltpu.VMEM),
            pl.BlockSpec(memory_space=pltpu.SMEM),
            pl.BlockSpec(memory_space=pltpu.SMEM),
        ],
        out_specs=pl.BlockSpec(memory_space=pl.ANY),
        scratch_shapes=[
            vmem((COMPS, 10, 16, 256), f32),
            vmem((2, 12, 16, 256), f32),
            vmem((10, 16, 256), f32),
            vmem((12, 16, 256), f32),
            vmem((2, COMPS, 16, 128), f32),
            vmem((2, 2, 16, 128), f32),
            vmem((2, 16, 128), f32),
            vmem((2, 16, 128), f32),
            vmem((16, 128), f32),
            vmem((9, 16, 128), f32),
            vmem((2, HOPS, 16, 256), f32),
            vmem((2, HOPS, 16, 128), f32),
            vmem((16, 128), f32),
            vmem((2, 16, 128), f32),
            vmem((13, 16, 128), f32),
            vmem((2, 13, 16, 128), f32),
            vmem((2, 16, 128), f32),
            vmem((2, 16, 128), f32),
            vmem((2, 16, 256), f32),
            vmem((2, 16, 256), f32),
            sems((2, HOPS)),
            sems((2, HOPS)),
            sems((2, HOPS)),
            sems((2, HOPS)),
            sems((5, 2)),
            sems((5, 2)),
            sems((2, 2)),
            sems((2, 2)),
            sems((2, 2)),
            sems((2, 2)),
            sems((INNER,)),
            sems((2,)),
        ],
        compiler_params=pltpu.CompilerParams(collective_id=0, has_side_effects=True),
        name="slab",
    )(state, jnp.swapaxes(tissue_mask, 1, 2), layer_index, fibre)


def solution(mesh):
    placed = (P(None, "gx", None, "gy"), P("gx", None, "gy"), P(), P())
    return jax.shard_map(
        shards, mesh=mesh, in_specs=placed, out_specs=P(None, "gx", None, "gy"), check_vma=False
    )
```

```python
import math

import jax
import jax.numpy as jnp
from jax import lax
from jax.experimental import pallas as pl
from jax.experimental.pallas import tpu as pltpu
from jax.sharding import PartitionSpec as P

STEPS = 8
TRANSVERSE = 0.04
LONGITUDINAL = 0.12
DT = 0.02
RTF = 8314.472 * 310.0 / 96485.3415
EK = RTF * math.log(5.4 / 138.3)
ENA = RTF * math.log(140.0 / 7.67)
EKS = RTF * math.log((5.4 + 0.03 * 140.0) / (138.3 + 0.03 * 7.67))
L2E = 1.0 / math.log(2.0)
KAPPA = -DT * L2E


def grow(volt, slope):
    return jnp.exp2(volt * (slope * L2E))


def sig(volt, centre, width):
    return jax.nn.sigmoid(volt * (1.0 / width) + (-centre / width))


def settle(gate, steady, factor):
    return steady + (gate - steady) * jnp.exp2(factor)


def membrane(s):
    x, m, h, j, d, f, r, z, p, q, w, ca = s
    v = x * 100.0
    over = v - EK
    b = grow(v, 0.05)
    ib = 1.0 / b
    b2 = b * b
    ib2 = ib * ib
    c = jnp.maximum(ca, 0.02)
    vca = (v - 0.5 * RTF * math.log(2000.0)) + (0.5 * RTF) * jnp.log(c)
    sodium = ((14.838 * m) * (m * m) * (h * j) + 0.00029) * (v - ENA)
    calcium = (0.08 * d * f + 0.000592) * vca
    sa = sig(v, EK + 200.0, -1.0 / 0.06)
    bk = (
        (30.0 * math.exp(0.0002 * (100.0 - EK))) * grow(v, 0.0002)
        + (10.0 * math.exp(0.1 * (-EK - 10.0))) * b2
    ) * sig(v, EK, 2.0)
    inward = 5.405 * sa / (sa + bk)
    potassium = (
        0.294 * r * z + 0.153 * p * q + inward + 0.0146 * sig(v, 25.0, 5.98)
    ) * over
    slow = (0.392 * w) * w * (v - EKS)
    en = grow(v, -1.0 / RTF)
    pump = (2.724 * 5.4 / 6.4 * 7.67 / 47.67) / (
        1.0 + 0.1245 * grow(v, -0.1 / RTF) + 0.0353 * en
    )
    ef = grow(v, 0.35 / RTF)
    eg = ef * en
    scale = 1000.0 / ((87.5**3 + 140.0**3) * 3.38)
    exchange = (
        (scale * 7.67**3 * 2.0) * ef - (scale * 2.5 * 140.0**3 * 0.001) * eg * c
    ) / (1.0 + 0.1 * eg)
    pump_ca = 0.1238 * c / (c + 0.5)
    total = sodium + calcium + potassium + slow + pump + exchange + pump_ca
    nx = x - (DT / 100.0) * total
    nca = ca - (DT * 0.05) * (calcium + pump_ca - 2.0 * exchange)
    low = 1.0 / (1.0 + math.exp(20.0) * grow(v, 0.5))
    nm = settle(
        m,
        sig(v, -56.86, 9.03) ** 2,
        (10.0 * KAPPA + (10.0 * KAPPA * math.exp(-12.0)) * (ib2 * ib2))
        / (sig(v, -35.0, -5.0) + sig(v, 50.0, -200.0)),
    )
    hs = sig(v, -71.55, -7.43)
    hs = hs * hs
    up = (KAPPA * 0.77 / 0.13) * sig(v, -10.66, 11.1)
    dn = (
        (KAPPA * 0.057 * math.exp(-80.0 / 6.8)) * grow(v, -1.0 / 6.8)
        + (KAPPA * 2.7) * grow(v, 0.079)
        + (KAPPA * 310000.0) * grow(v, 0.3485)
    )
    nh = settle(h, hs, up + low * (dn - up))
    up = (KAPPA * 0.6) * grow(v, 0.057) * sig(v, -32.0, 10.0)
    dn = ((KAPPA * -25428.0) * grow(v, 0.2444) - (KAPPA * 6.948e-06) * grow(v, -0.04391)) * (
        v + 37.78
    ) * sig(v, -79.23, -1.0 / 0.311) + (KAPPA * 0.02424) * grow(v, -0.01052) * sig(
        v, -40.14, 1.0 / 0.1378
    )
    nj = settle(j, hs, up + low * (dn - up))
    nd = settle(
        d,
        sig(v, -8.0, 7.5),
        KAPPA
        / ((1.96 * sig(v, -35.0, 13.0) + 0.35) * sig(v, -5.0, -5.0) + sig(v, 50.0, 20.0)),
    )
    t = v + 27.0
    nf = settle(
        f,
        sig(v, -20.0, -7.0),
        1.0
        / (
            (1102.5 / KAPPA) * jnp.exp2(t * t * (-L2E / 225.0))
            + (200.0 / KAPPA) * sig(v, 13.0, 10.0)
            + (180.0 / KAPPA) * sig(v, -30.0, -10.0)
            + 20.0 / KAPPA
        ),
    )
    t = v + 40.0
    nr = settle(
        r,
        sig(v, 20.0, 6.0),
        1.0 / ((9.5 / KAPPA) * jnp.exp2(t * t * (-L2E / 1800.0)) + 0.8 / KAPPA),
    )
    t = v + 45.0
    nz = settle(
        z,
        sig(v, -20.0, -5.0),
        1.0
        / (
            (85.0 / KAPPA) * jnp.exp2(t * t * (-L2E / 320.0))
            + (5.0 / KAPPA) * sig(v, 20.0, -5.0)
            + 3.0 / KAPPA
        ),
    )
    k = KAPPA / 2700.0
    np_ = settle(
        p,
        sig(v, -26.0, 7.0),
        (k + (k * math.exp(-4.5)) * ib2)
        * (1.0 + math.exp(30.0 / 11.5) * grow(v, 1.0 / 11.5)),
    )
    k = KAPPA / 3.36
    nq = settle(
        q,
        sig(v, -88.0, -24.0),
        (k * (1.0 + math.exp(-6.0))) + (k * math.exp(-3.0)) * (b + ib),
    )
    nw = settle(
        w,
        sig(v, -5.0, 14.0),
        1.0
        / (
            lax.rsqrt(1.0 + math.exp(5.0 / 6.0) * grow(v, -1.0 / 6.0))
            * ((1400.0 / KAPPA) * sig(v, 35.0, -15.0))
            + 80.0 / KAPPA
        ),
    )
    return nx, nm, nh, nj, nd, nf, nr, nz, np_, nq, nw, nca


INNER = 8
COMPS = 12
HOPS = STEPS - 1
MESH = pl.DeviceIdType.MESH


def react(state, inside):
    fresh = membrane(state)
    return [jnp.where(inside, new, old) for new, old in zip(fresh, state)]


def lanes():
    return lax.broadcasted_iota(jnp.int32, (16, 128), 1)


def turn(tile, shift):
    shift = shift % 128
    return tile if shift == 0 else pltpu.roll(tile, shift, 1)


def coefficients(layer_ref, fibre_ref, coef):
    row = lax.broadcasted_iota(jnp.int32, (16, 128), 0)
    angle_in = jnp.zeros((16, 128), jnp.float32)
    angle_out = jnp.zeros((16, 128), jnp.float32)
    for level in range(16):
        layer = layer_ref[level]
        angle_in = jnp.where(row == level, fibre_ref[0, layer], angle_in)
        angle_out = jnp.where(row == level, fibre_ref[1, layer], angle_out)
    along_x = jnp.cos(angle_in) * jnp.cos(angle_out)
    along_y = jnp.sin(angle_in) * jnp.cos(angle_out)
    along_z = jnp.sin(angle_out)
    spread = LONGITUDINAL - TRANSVERSE
    coef[0] = TRANSVERSE + spread * along_x * along_x
    coef[1] = TRANSVERSE + spread * along_y * along_y
    coef[2] = spread * along_x * along_y / 2.0
    parts = (
        TRANSVERSE + spread * along_z * along_z,
        spread * along_x * along_z / 2.0,
        spread * along_y * along_z / 2.0,
    )
    for index, part in enumerate(parts):
        below = (part + pltpu.roll(part, 1, 0)) / 2.0
        above = (part + pltpu.roll(part, 15, 0)) / 2.0
        coef[3 + index] = jnp.where(row == 0, 0.0, below)
        coef[6 + index] = jnp.where(row == 15, 0.0, above)


def lift(tile):
    return pltpu.roll(tile, 15, 0)


def sink(tile):
    return pltpu.roll(tile, 1, 0)


def terms(coef, value, above, below):
    across = above - below
    flat = coef[1] * value
    tilt = coef[2] * across + lift(coef[5] * value) - sink(coef[8] * value)
    rest = (
        coef[0] * (above + below)
        + lift(coef[3] * value + coef[4] * across)
        + sink(coef[6] * value - coef[7] * across)
    )
    return rest, flat + tilt, flat - tilt


def plane_totals(coef, here, above, below, parts, base):
    lane = lanes()
    first, second = (terms(coef, *tiles) for tiles in zip(here, above, below))
    after_first, after_second = pltpu.roll(first[1], 127, 1), pltpu.roll(second[1], 127, 1)
    before_first, before_second = pltpu.roll(first[2], 1, 1), pltpu.roll(second[2], 1, 1)
    enter_low, enter_high = turn(parts[2], -(base + 7)), turn(parts[1], 127 - (base + 8))
    low, high = lane == 0, lane == 127
    totals = (
        first[0]
        + jnp.where(high, after_second, after_first)
        + jnp.where(low, enter_low, before_first),
        second[0]
        + jnp.where(high, enter_high, after_second)
        + jnp.where(low, before_first, before_second),
    )
    return totals, turn(first[1], base + 7), turn(second[2], base + 9)


def strip_total(parts, border):
    column = lax.rem(lanes(), 16)
    after = jnp.where(column == 7, border[0], pltpu.roll(parts[1], 127, 1))
    before = jnp.where(column == 8, border[1], pltpu.roll(parts[2], 1, 1))
    return parts[0] + after + before


def kernel(
    state_ref,
    mask_ref,
    layer_ref,
    fibre_ref,
    cells,
    packed,
    keep,
    mask,
    strip_cells,
    strip_packed,
    strip_keep,
    strip_mask,
    far_mask,
    borders,
    coef,
    hop_in,
    hop_strip_in,
    strip_out,
    spread_out,
    spread_in,
    side_out,
    side_in,
    relay_out,
    relay_in,
    relay_gates_out,
    relay_gates_in,
    hop_send,
    hop_recv,
    strip_send,
    strip_recv,
    lead_send,
    lead_recv,
    side_send,
    side_recv,
    relay_send,
    relay_recv,
    load_sem,
):
    me_x, me_y = lax.axis_index("gx"), lax.axis_index("gy")
    size_x, size_y = lax.axis_size("gx"), lax.axis_size("gy")
    along_x = ((me_x + 1, me_y), (me_x - 1, me_y))
    along_y = ((me_x, me_y + 1), (me_x, me_y - 1))
    ends_x = (me_x < size_x - 1, me_x > 0)
    ends_y = (me_y < size_y - 1, me_y > 0)
    ways = (0, 1)

    def sending(ends, way, action):
        pl.when(ends[way])(action)

    def receiving(ends, way, action):
        pl.when(ends[1 - way])(action)

    barrier = pltpu.get_barrier_semaphore()
    for ends, targets in ((ends_x, along_x), (ends_y, along_y)):
        for way in ways:

            def greet(target=targets[way]):
                pl.semaphore_signal(barrier, inc=1, device_id=target, device_id_type=MESH)

            sending(ends, way, greet)

    corners = [(way_x, way_y) for way_x in ways for way_y in ways]

    def diagonal(way_x, way_y):
        return along_x[way_x][0], along_y[way_y][1]

    for way_x, way_y in corners:

        @pl.when(ends_x[way_x] & ends_y[way_y])
        def _(target=diagonal(way_x, way_y)):
            pl.semaphore_signal(barrier, inc=1, device_id=target, device_id_type=MESH)

    def remote(source, target, sends, recvs, device):
        return pltpu.make_async_remote_copy(
            src_ref=source,
            dst_ref=target,
            send_sem=sends,
            recv_sem=recvs,
            device_id=device,
            device_id_type=MESH,
        )

    def load(plane):
        return pltpu.make_async_copy(
            state_ref.at[:, plane], cells.at[:, plane + 1], load_sem.at[plane]
        )

    for plane in (0, 7, 1, 6, 2, 5, 3, 4):
        load(plane).start()

    lane = lanes()
    coefficients(layer_ref, fibre_ref, coef)
    spread_tile = jnp.zeros((16, 128), jnp.float32)
    unit = (
        lax.broadcasted_iota(jnp.int32, (16, 16), 0) == lax.broadcasted_iota(jnp.int32, (16, 16), 1)
    ).astype(jnp.float32)
    for plane in range(INNER):
        blocks = lax.dot_general(
            unit,
            (mask_ref[plane] > 0).astype(jnp.float32),
            (((1,), (1,)), ((), ())),
            preferred_element_type=jnp.float32,
        )
        for half in range(2):
            tile = jnp.broadcast_to(blocks[:, half : half + 1], (16, 128))
            mask[plane + 2, :, half * 128 : half * 128 + 128] = tile
            spread_tile = jnp.where(lane == 2 * plane + half, tile, spread_tile)
    spread_out[...] = spread_tile

    for way in ways:

        @pl.when(jnp.logical_not(ends_x[1 - way]))
        def _(way=way):
            for step in range(HOPS):
                hop_in[way, step] = jnp.zeros((16, 256), jnp.float32)
                hop_strip_in[way, step] = jnp.zeros((16, 128), jnp.float32)
            spread_in[way] = jnp.zeros((16, 128), jnp.float32)
            for comp in range(COMPS):
                cells[comp, 0 if way == 0 else 9] = jnp.zeros((16, 256), jnp.float32)

        @pl.when(jnp.logical_not(ends_y[1 - way]))
        def _(way=way):
            for index in range(7):
                side_in[way, index] = jnp.zeros((16, 128), jnp.float32)

    for way_x, way_y in corners:

        @pl.when(jnp.logical_not(ends_x[1 - way_x] & ends_y[1 - way_y]))
        def _(slot=(way_x, way_y)):
            relay_in[slot] = jnp.zeros((16, 128), jnp.float32)
            relay_gates_in[slot] = jnp.zeros((16, 256), jnp.float32)

    def react_plane(slot, parity):
        for top in (0, 8):
            rows = pl.ds(top, 8)
            inside = mask[slot + 1, rows] > 0.0
            fresh = react([cells[comp, slot, rows] for comp in range(COMPS)], inside)
            for comp in range(COMPS):
                cells[comp, slot, rows] = fresh[comp]
            packed[parity, slot + 1, rows] = jnp.where(inside, fresh[0], 0.0)

    body = (lane >= 16) & (lane < 112)
    tips = jnp.logical_not(body)
    every = lane >= 0

    def react_strip(which, parity, region):
        for top in (0, 8):
            rows = pl.ds(top, 8)
            inside = strip_mask[which, rows] > 0.0
            fresh = react(
                [strip_cells[which, comp, rows] for comp in range(COMPS)], inside & region[0:8]
            )
            for comp in range(COMPS):
                strip_cells[which, comp, rows] = fresh[comp]
            strip_packed[parity, which, rows] = jnp.where(
                region[0:8], jnp.where(inside, fresh[0], 0.0), strip_packed[parity, which, rows]
            )

    def react_pair(pair, parity):
        react_plane(pair + 1, parity)
        react_plane(8 - pair, parity)

    def first_pair(pair, carry):
        load(pair).wait()
        load(7 - pair).wait()
        react_pair(pair, 0)
        return carry

    lax.fori_loop(0, 4, first_pair, 0)

    inner_half = lax.rem(lane, 16) < 8

    def pack_side(read):
        tile = jnp.zeros((16, 128), jnp.float32)
        for plane in range(INNER):
            first, second = read(plane)
            base = plane * 16
            both = turn(jnp.where(lane < 64, first, second), base + 8)
            tile = jnp.where((lane >= base) & (lane < base + 16), both, tile)
        return tile

    def own(comp):
        return lambda plane: (cells[comp, plane + 1, :, 0:128], cells[comp, plane + 1, :, 128:256])

    own_mask = pack_side(lambda plane: (mask[plane + 2, :, 0:128], mask[plane + 2, :, 128:256]))
    sides = [pack_side(own(0)), own_mask] + [pack_side(own(comp)) for comp in range(1, COMPS)]
    for index in range(7):
        even = sides[2 * index]
        odd = sides[2 * index + 1] if index < 6 else even
        side_out[0, index] = jnp.where(inner_half, even, turn(odd, 8))
        side_out[1, index] = jnp.where(inner_half, turn(odd, -8), even)
    for way, (edge, inward) in enumerate(((7, 6), (0, 1))):
        tile = jnp.zeros((16, 128), jnp.float32)
        parts = (
            (sides[0], edge),
            (own_mask, edge),
            (own_mask, inward),
            (sides[0] * own_mask, inward),
        )
        for group, (part, plane) in enumerate(parts):
            here = (lane >= group * 16) & (lane < group * 16 + 16)
            tile = jnp.where(here, turn(part, group * 16 - plane * 16), tile)
        relay_out[way] = tile
        for half, gates in enumerate((range(1, 9), range(9, 12))):
            tile = jnp.zeros((16, 128), jnp.float32)
            for group, comp in enumerate(gates):
                here = (lane >= group * 16) & (lane < group * 16 + 16)
                tile = jnp.where(here, turn(sides[comp + 1], group * 16 - edge * 16), tile)
            relay_gates_out[way, :, half * 128 : half * 128 + 128] = tile

    peers_x = sum(end.astype(jnp.int32) for end in ends_x)
    peers_y = sum(end.astype(jnp.int32) for end in ends_y)
    peers = peers_x + peers_y + peers_x * peers_y
    pl.semaphore_wait(barrier, peers)

    early, late, lead, bulk = [], [], [], []
    for way, (edge, inward, slot) in enumerate(((7, 6, 0), (0, 1, 9))):
        early.append(
            remote(
                side_out.at[way, 0],
                side_in.at[way, 0],
                side_send.at[0, way],
                side_recv.at[0, way],
                along_y[way],
            )
        )
        late.append(
            remote(
                side_out.at[way, pl.ds(1, 6)],
                side_in.at[way, pl.ds(1, 6)],
                side_send.at[1, way],
                side_recv.at[1, way],
                along_y[way],
            )
        )
        lead.append(
            [
                remote(
                    source, target, lead_send.at[index, way], lead_recv.at[index, way], along_x[way]
                )
                for index, (source, target) in enumerate(
                    (
                        (cells.at[0, edge + 1], cells.at[0, slot]),
                        (packed.at[0, inward + 2], hop_in.at[way, 0]),
                        (spread_out, spread_in.at[way]),
                    )
                )
            ]
        )
        bulk.append(
            [
                remote(
                    cells.at[pl.ds(start, size), edge + 1],
                    cells.at[pl.ds(start, size), slot],
                    lead_send.at[index, way],
                    lead_recv.at[index, way],
                    along_x[way],
                )
                for index, start, size in ((3, 1, 11),)
            ]
        )
    def corner_copy(way_x, way_y, index):
        source, target = ((relay_out, relay_in), (relay_gates_out, relay_gates_in))[index]
        return remote(
            source.at[way_x],
            target.at[way_x, way_y],
            relay_send.at[index, way_x, way_y],
            relay_recv.at[index, way_x, way_y],
            diagonal(way_x, way_y),
        )

    def corner_start(index):
        for way_x, way_y in corners:

            @pl.when(ends_x[way_x] & ends_y[way_y])
            def _(way_x=way_x, way_y=way_y):
                corner_copy(way_x, way_y, index).start()

    def corner_sent(index):
        for way_x, way_y in corners:

            @pl.when(ends_x[way_x] & ends_y[way_y])
            def _(way_x=way_x, way_y=way_y):
                corner_copy(way_x, way_y, index).wait_send()

    def corner_wait(index):
        for way_x, way_y in corners:

            @pl.when(ends_x[1 - way_x] & ends_y[1 - way_y])
            def _(way_x=way_x, way_y=way_y):
                corner_copy(way_x, way_y, index).wait_recv()

    corner_start(0)
    for way in ways:
        sending(ends_y, way, early[way].start)
    for way in ways:
        for copy in lead[way]:
            sending(ends_x, way, copy.start)
    for way in ways:
        sending(ends_y, way, late[way].start)
    corner_start(1)
    for way in ways:
        for copy in bulk[way]:
            sending(ends_x, way, copy.start)

    def unpack(index):
        even = jnp.where(inner_half, side_in[0, index], side_in[1, index])
        odd = jnp.where(inner_half, turn(side_in[0, index], -8), turn(side_in[1, index], 8))
        return even, odd

    for way in ways:
        receiving(ends_y, way, early[way].wait_recv)
    strip_cells[0, 0], strip_mask[0] = unpack(0)
    strip_packed[0, 0] = strip_mask[0] * strip_cells[0, 0]

    def load_factors():
        return [coef[index] for index in range(9)]

    def sum_planes(factors, read, planes, parts, border, emit):
        leave_low, leave_high = border
        for plane, base, around in planes:
            below, above = around or (read(plane - 1), read(plane + 1))
            totals, low, high = plane_totals(factors, read(plane), above, below, parts, base)
            for half in range(2):
                emit(plane, half, totals[half])
            leave_low = jnp.where(lane == base + 7, low, leave_low)
            leave_high = jnp.where(lane == base + 8, high, leave_high)
        return leave_low, leave_high

    empty = jnp.zeros((16, 128), jnp.float32)

    def inner_sums(read, strip, kept, emit):
        factors = load_factors()
        parts = terms(factors, strip, turn(strip, 112), turn(strip, 16))
        planes = [(plane, 16 * plane, None) for plane in range(2, INNER - 2)]
        border = sum_planes(factors, read, planes, parts, (empty, empty), emit)
        for index, tile in enumerate(border):
            borders[kept, index] = tile

    def middle_sums(read, strip, kept, emit, emit_strip):
        factors = load_factors()
        parts = terms(factors, strip, turn(strip, 112), turn(strip, 16))
        planes = [(plane, 16 * plane, None) for plane in (1, INNER - 2)]
        border = borders[kept, 0], borders[kept, 1]
        border = sum_planes(factors, read, planes, parts, border, emit)
        emit_strip(strip_total(parts, border))

    def edge_sums(read, strips, emit, emit_strip):
        factors = load_factors()
        strip, outer = strips
        above = jnp.where(lane >= 112, turn(outer, 96), turn(strip, 112))
        below = jnp.where(lane < 16, outer, turn(strip, 16))
        parts = terms(factors, strip, above, below)
        planes = [(plane, 16 * plane, None) for plane in (0, INNER - 1)]
        border = sum_planes(factors, read, planes, parts, (empty, empty), emit)
        if emit_strip is not None:
            emit_strip(strip_total(parts, border))

    def rim_sums(read, strips, far, emit, emit_strip):
        factors = load_factors()
        strip, outer = strips
        beyond = empty
        planes = []
        for way, (rim, near) in enumerate(((-1, 0), (INNER, INNER - 1))):
            first, second, far_strip, base = far(way)
            place = way * 16
            here = (lane >= place) & (lane < place + 16)
            beyond = jnp.where(here, turn(far_strip, place - base), beyond)
            pair = ((first, second), read(near))
            planes.append((rim, place, pair if way == 0 else pair[::-1]))
        lower = lane < 16
        near = jnp.where(lower, strip, turn(strip, 32))
        parts = terms(
            factors, outer, jnp.where(lower, near, beyond), jnp.where(lower, beyond, near)
        )
        border = sum_planes(factors, read, planes, parts, (empty, empty), emit)
        emit_strip(strip_total(parts, border))

    def mask_tiles(plane):
        return mask[plane + 2, :, 0:128], mask[plane + 2, :, 128:256]

    def keep_plane(plane, half, total):
        columns = slice(half * 128, half * 128 + 128)
        keep[plane + 1, :, columns] = 1.0 - mask[plane + 2, :, columns] * total

    def keep_strip(which, region):
        def emit(total):
            strip_keep[which] = jnp.where(
                region, 1.0 - strip_mask[which] * total, strip_keep[which]
            )

        return emit

    def mask_far(way):
        return (*mask_tiles(-2 if way == 0 else 9), far_mask[...], way * 16)

    def move_plane(plane, half, total):
        columns = slice(half * 128, half * 128 + 128)
        cells[0, plane + 1, :, columns] = (
            cells[0, plane + 1, :, columns] * keep[plane + 1, :, columns]
            + mask[plane + 2, :, columns] * total
        )

    def move_strip(which, region):
        def emit(total):
            value = strip_cells[which, 0]
            moved = value * strip_keep[which] + strip_mask[which] * total
            strip_cells[which, 0] = jnp.where(region, moved, value)

        return emit

    def tiles(parity):
        return lambda plane: (
            packed[parity, plane + 2, :, 0:128],
            packed[parity, plane + 2, :, 128:256],
        )

    def strips_of(parity):
        return strip_packed[parity, 0], strip_packed[parity, 1]

    def hop(way, step, parity):
        return remote(
            packed.at[parity, 8 if way == 0 else 3],
            hop_in.at[way, step],
            hop_send.at[way, step],
            hop_recv.at[way, step],
            along_x[way],
        )

    def strip_hop(way, step, parity):
        return remote(
            strip_out.at[parity],
            hop_strip_in.at[way, step],
            strip_send.at[way, step],
            strip_recv.at[way, step],
            along_x[way],
        )

    def rim_step(step, parity):
        def far(way):
            return (
                hop_in[way, step - 1, :, 0:128],
                hop_in[way, step - 1, :, 128:256],
                hop_strip_in[way, step - 1],
                96 if way == 0 else 16,
            )

        read, strips = tiles(parity), strips_of(parity)
        rim_sums(read, strips, far, move_plane, move_strip(1, every))

    def rim_planes(parity):
        react_plane(0, parity)
        react_plane(9, parity)

    def open_rim():
        corner_wait(0)
        for way in ways:
            for copy in lead[way]:
                receiving(ends_x, way, copy.wait_recv)
        outer_mask = jnp.zeros((16, 128), jnp.float32)
        outer_far_mask = jnp.zeros((16, 128), jnp.float32)
        outer_first = jnp.zeros((16, 128), jnp.float32)
        for way, (edge, inward, slot, beyond) in enumerate(((7, 6, 1, 0), (0, 1, 10, 11))):
            for half in range(2):
                columns = slice(half * 128, half * 128 + 128)
                for plane, target in ((edge, slot), (inward, beyond)):
                    index = 2 * plane + half
                    mask[target, :, columns] = jnp.broadcast_to(
                        spread_in[way, :, index : index + 1], (16, 128)
                    )
            packed[0, slot] = mask[slot] * cells[0, slot - 1]
            place = way * 16
            here = (lane >= place) & (lane < place + 16)
            relayed = jnp.where(inner_half, relay_in[way, 0], relay_in[way, 1])
            outer_first = jnp.where(here, turn(relayed, place), outer_first)
            outer_mask = jnp.where(here, turn(relayed, place - 16), outer_mask)
            outer_far_mask = jnp.where(here, turn(relayed, place - 32), outer_far_mask)
            hop_strip_in[way, 0] = turn(relayed, inward * 16 - 48)
        strip_cells[1, 0] = outer_first
        strip_mask[1] = outer_mask
        strip_packed[0, 1] = outer_mask * outer_first
        far_mask[...] = outer_far_mask
        masks = (strip_mask[0], outer_mask)
        edge_sums(mask_tiles, masks, keep_plane, keep_strip(0, tips))
        rim_sums(mask_tiles, masks, mask_far, keep_plane, keep_strip(1, every))

    def open_rim_gates():
        corner_wait(1)
        for way in ways:
            for copy in bulk[way]:
                receiving(ends_x, way, copy.wait_recv)
        for half, gates in enumerate((range(1, 9), range(9, 12))):
            for group, comp in enumerate(gates):
                tile = jnp.zeros((16, 128), jnp.float32)
                for way in ways:
                    place = way * 16
                    here = (lane >= place) & (lane < place + 16)
                    columns = slice(half * 128, half * 128 + 128)
                    source = jnp.where(
                        inner_half,
                        relay_gates_in[way, 0, :, columns],
                        relay_gates_in[way, 1, :, columns],
                    )
                    tile = jnp.where(here, turn(source, place - group * 16), tile)
                strip_cells[1, comp] = tile

    def open_strip_gates():
        for way in ways:
            receiving(ends_y, way, late[way].wait_recv)
        for index in range(1, 7):
            even, odd = unpack(index)
            strip_cells[0, 2 * index - 1] = even
            if index < 6:
                strip_cells[0, 2 * index] = odd

    inner_sums(mask_tiles, strip_mask[0], 0, keep_plane)
    middle_sums(mask_tiles, strip_mask[0], 0, keep_plane, keep_strip(0, body))
    inner_sums(tiles(0), strip_packed[0, 0], 1, move_plane)

    def advance(step):
        first, second = (isinstance(step, int) and step == value for value in (1, 2))
        now = lax.rem(step, 2)
        old = 1 - now
        if not (first or second):
            for way in ways:
                sending(ends_x, way, hop(way, step - 2, now).wait_send)
                sending(ends_x, way, strip_hop(way, step - 2, now).wait_send)
        middle_sums(tiles(old), strip_packed[old, 0], 1, move_plane, move_strip(0, body))
        if not second:
            react_pair(3, now)
        if first:
            open_strip_gates()
        react_strip(0, now, body)
        strip_out[now] = strip_packed[now, 0]
        react_pair(1, now)

        @pl.when(step < HOPS)
        def _():
            for way in ways:
                sending(ends_x, way, hop(way, step, now).start)
                sending(ends_x, way, strip_hop(way, step, now).start)

        if first:
            react_pair(2, now)
            inner_sums(tiles(now), strip_packed[now, 0], 1, move_plane)
            react_pair(3, old)
            react_pair(2, old)
            open_rim()
            for way in ways:
                for copy in lead[way] + bulk[way]:
                    sending(ends_x, way, copy.wait_send)
        elif second:
            open_rim_gates()
        else:
            for way in ways:
                for copy in (hop(way, step - 2, now), strip_hop(way, step - 2, now)):
                    receiving(ends_x, way, copy.wait_recv)
        if not first:
            rim_step(step - 1, now)
            if not second:
                react_pair(2, now)
            react_strip(1, old, every)
            rim_planes(old)
        edge_sums(tiles(old), strips_of(old), move_plane, move_strip(0, tips))
        react_strip(0, now, tips)
        if not first:
            inner_sums(tiles(now), strip_packed[now, 0], 1, move_plane)
        react_pair(0, now)

    advance(1)
    advance(2)

    def later(step, carry):
        advance(step)
        return carry

    lax.fori_loop(3, STEPS, later, 0)

    last = (STEPS - 1) % 2
    middle_sums(tiles(last), strip_packed[last, 0], 1, move_plane, lambda total: None)
    for way in ways:
        for copy in (hop(way, HOPS - 1, 1 - last), strip_hop(way, HOPS - 1, 1 - last)):
            receiving(ends_x, way, copy.wait_recv)
    rim_step(STEPS - 1, 1 - last)
    react_strip(1, last, every)
    rim_planes(last)
    edge_sums(tiles(last), strips_of(last), move_plane, None)
    corner_sent(0)
    corner_sent(1)
    for way in ways:
        for copy in (hop(way, HOPS - 1, 1 - last), strip_hop(way, HOPS - 1, 1 - last)):
            sending(ends_x, way, copy.wait_send)
        sending(ends_y, way, early[way].wait_send)
        sending(ends_y, way, late[way].wait_send)


def unload(cells, out_ref, store_sem):
    stores = [
        pltpu.make_async_copy(
            cells.at[comp, pl.ds(1, INNER)], out_ref.at[comp], store_sem.at[comp]
        )
        for comp in range(COMPS)
    ]
    for copy in stores:
        copy.start()
    for copy in stores:
        copy.wait()


def shards(state, tissue_mask, layer_index, fibre):
    vmem, sems = pltpu.VMEM, pltpu.SemaphoreType.DMA
    f32 = jnp.float32
    cells = pl.pallas_call(
        kernel,
        out_shape=vmem((COMPS, 10, 16, 256), f32),
        in_specs=[
            pl.BlockSpec(memory_space=pl.ANY),
            pl.BlockSpec(memory_space=pltpu.VMEM),
            pl.BlockSpec(memory_space=pltpu.SMEM),
            pl.BlockSpec(memory_space=pltpu.SMEM),
        ],
        out_specs=pl.BlockSpec(memory_space=pltpu.VMEM),
        scratch_shapes=[
            vmem((2, 12, 16, 256), f32),
            vmem((10, 16, 256), f32),
            vmem((12, 16, 256), f32),
            vmem((2, COMPS, 16, 128), f32),
            vmem((2, 2, 16, 128), f32),
            vmem((2, 16, 128), f32),
            vmem((2, 16, 128), f32),
            vmem((16, 128), f32),
            vmem((2, 4, 16, 128), f32),
            vmem((9, 16, 128), f32),
            vmem((2, HOPS, 16, 256), f32),
            vmem((2, HOPS, 16, 128), f32),
            vmem((2, 16, 128), f32),
            vmem((16, 128), f32),
            vmem((2, 16, 128), f32),
            vmem((2, 7, 16, 128), f32),
            vmem((2, 7, 16, 128), f32),
            vmem((2, 16, 128), f32),
            vmem((2, 2, 16, 128), f32),
            vmem((2, 16, 256), f32),
            vmem((2, 2, 16, 256), f32),
            sems((2, HOPS)),
            sems((2, HOPS)),
            sems((2, HOPS)),
            sems((2, HOPS)),
            sems((4, 2)),
            sems((4, 2)),
            sems((2, 2)),
            sems((2, 2)),
            sems((2, 2, 2)),
            sems((2, 2, 2)),
            sems((INNER,)),
        ],
        compiler_params=pltpu.CompilerParams(collective_id=0, has_side_effects=True, vmem_limit_bytes=64000000),
        name="slab",
    )(state, jnp.swapaxes(tissue_mask, 1, 2), layer_index, fibre)
    return pl.pallas_call(
        unload,
        out_shape=jax.ShapeDtypeStruct(state.shape, f32),
        in_specs=[pl.BlockSpec(memory_space=pl.ANY)],
        out_specs=pl.BlockSpec(memory_space=pl.ANY),
        scratch_shapes=[sems((COMPS,))],
        compiler_params=pltpu.CompilerParams(vmem_limit_bytes=1 << 20),
        name="unload",
    )(cells)


def solution(mesh):
    placed = (P(None, "gx", None, "gy"), P("gx", None, "gy"), P(), P())
    return jax.shard_map(
        shards, mesh=mesh, in_specs=placed, out_specs=P(None, "gx", None, "gy"), check_vma=False
    )
```

```python
import math

import jax
import jax.numpy as jnp
from jax import lax
from jax.experimental import pallas as pl
from jax.experimental.pallas import tpu as pltpu
from jax.sharding import PartitionSpec as P

STEPS = 8
TRANSVERSE = 0.04
LONGITUDINAL = 0.12
DT = 0.02
RTF = 8314.472 * 310.0 / 96485.3415
EK = RTF * math.log(5.4 / 138.3)
ENA = RTF * math.log(140.0 / 7.67)
EKS = RTF * math.log((5.4 + 0.03 * 140.0) / (138.3 + 0.03 * 7.67))
L2E = 1.0 / math.log(2.0)
KAPPA = -DT * L2E


def grow(volt, slope):
    return jnp.exp2(volt * (slope * L2E))


def sig(volt, centre, width):
    return jax.nn.sigmoid(volt * (1.0 / width) + (-centre / width))


def settle(gate, steady, factor):
    return steady + (gate - steady) * jnp.exp2(factor)


def membrane(s):
    x, m, h, j, d, f, r, z, p, q, w, ca = s
    v = x * 100.0
    over = v - EK
    b = grow(v, 0.05)
    ib = 1.0 / b
    b2 = b * b
    ib2 = ib * ib
    c = jnp.maximum(ca, 0.02)
    vca = (v - 0.5 * RTF * math.log(2000.0)) + (0.5 * RTF) * jnp.log(c)
    sodium = ((14.838 * m) * (m * m) * (h * j) + 0.00029) * (v - ENA)
    calcium = (0.08 * d * f + 0.000592) * vca
    sa = sig(v, EK + 200.0, -1.0 / 0.06)
    bk = (
        (30.0 * math.exp(0.0002 * (100.0 - EK))) * grow(v, 0.0002)
        + (10.0 * math.exp(0.1 * (-EK - 10.0))) * b2
    ) * sig(v, EK, 2.0)
    inward = 5.405 * sa / (sa + bk)
    potassium = (
        0.294 * r * z + 0.153 * p * q + inward + 0.0146 * sig(v, 25.0, 5.98)
    ) * over
    slow = (0.392 * w) * w * (v - EKS)
    en = grow(v, -1.0 / RTF)
    pump = (2.724 * 5.4 / 6.4 * 7.67 / 47.67) / (
        1.0 + 0.1245 * grow(v, -0.1 / RTF) + 0.0353 * en
    )
    ef = grow(v, 0.35 / RTF)
    eg = ef * en
    scale = 1000.0 / ((87.5**3 + 140.0**3) * 3.38)
    exchange = (
        (scale * 7.67**3 * 2.0) * ef - (scale * 2.5 * 140.0**3 * 0.001) * eg * c
    ) / (1.0 + 0.1 * eg)
    pump_ca = 0.1238 * c / (c + 0.5)
    total = sodium + calcium + potassium + slow + pump + exchange + pump_ca
    nx = x - (DT / 100.0) * total
    nca = ca - (DT * 0.05) * (calcium + pump_ca - 2.0 * exchange)
    low = 1.0 / (1.0 + math.exp(20.0) * grow(v, 0.5))
    nm = settle(
        m,
        sig(v, -56.86, 9.03) ** 2,
        (10.0 * KAPPA + (10.0 * KAPPA * math.exp(-12.0)) * (ib2 * ib2))
        / (sig(v, -35.0, -5.0) + sig(v, 50.0, -200.0)),
    )
    hs = sig(v, -71.55, -7.43)
    hs = hs * hs
    up = (KAPPA * 0.77 / 0.13) * sig(v, -10.66, 11.1)
    dn = (
        (KAPPA * 0.057 * math.exp(-80.0 / 6.8)) * grow(v, -1.0 / 6.8)
        + (KAPPA * 2.7) * grow(v, 0.079)
        + (KAPPA * 310000.0) * grow(v, 0.3485)
    )
    nh = settle(h, hs, up + low * (dn - up))
    up = (KAPPA * 0.6) * grow(v, 0.057) * sig(v, -32.0, 10.0)
    dn = ((KAPPA * -25428.0) * grow(v, 0.2444) - (KAPPA * 6.948e-06) * grow(v, -0.04391)) * (
        v + 37.78
    ) * sig(v, -79.23, -1.0 / 0.311) + (KAPPA * 0.02424) * grow(v, -0.01052) * sig(
        v, -40.14, 1.0 / 0.1378
    )
    nj = settle(j, hs, up + low * (dn - up))
    nd = settle(
        d,
        sig(v, -8.0, 7.5),
        KAPPA
        / ((1.96 * sig(v, -35.0, 13.0) + 0.35) * sig(v, -5.0, -5.0) + sig(v, 50.0, 20.0)),
    )
    t = v + 27.0
    nf = settle(
        f,
        sig(v, -20.0, -7.0),
        1.0
        / (
            (1102.5 / KAPPA) * jnp.exp2(t * t * (-L2E / 225.0))
            + (200.0 / KAPPA) * sig(v, 13.0, 10.0)
            + (180.0 / KAPPA) * sig(v, -30.0, -10.0)
            + 20.0 / KAPPA
        ),
    )
    t = v + 40.0
    nr = settle(
        r,
        sig(v, 20.0, 6.0),
        1.0 / ((9.5 / KAPPA) * jnp.exp2(t * t * (-L2E / 1800.0)) + 0.8 / KAPPA),
    )
    t = v + 45.0
    nz = settle(
        z,
        sig(v, -20.0, -5.0),
        1.0
        / (
            (85.0 / KAPPA) * jnp.exp2(t * t * (-L2E / 320.0))
            + (5.0 / KAPPA) * sig(v, 20.0, -5.0)
            + 3.0 / KAPPA
        ),
    )
    k = KAPPA / 2700.0
    np_ = settle(
        p,
        sig(v, -26.0, 7.0),
        (k + (k * math.exp(-4.5)) * ib2)
        * (1.0 + math.exp(30.0 / 11.5) * grow(v, 1.0 / 11.5)),
    )
    k = KAPPA / 3.36
    nq = settle(
        q,
        sig(v, -88.0, -24.0),
        (k * (1.0 + math.exp(-6.0))) + (k * math.exp(-3.0)) * (b + ib),
    )
    nw = settle(
        w,
        sig(v, -5.0, 14.0),
        1.0
        / (
            lax.rsqrt(1.0 + math.exp(5.0 / 6.0) * grow(v, -1.0 / 6.0))
            * ((1400.0 / KAPPA) * sig(v, 35.0, -15.0))
            + 80.0 / KAPPA
        ),
    )
    return nx, nm, nh, nj, nd, nf, nr, nz, np_, nq, nw, nca


INNER = 8
COMPS = 12
HOPS = STEPS - 1
MESH = pl.DeviceIdType.MESH


def react(state, inside):
    fresh = membrane(state)
    return [jnp.where(inside, new, old) for new, old in zip(fresh, state)]


def lanes():
    return lax.broadcasted_iota(jnp.int32, (16, 128), 1)


def turn(tile, shift):
    shift = shift % 128
    return tile if shift == 0 else pltpu.roll(tile, shift, 1)


def coefficients(layer_ref, fibre_ref, coef):
    row = lax.broadcasted_iota(jnp.int32, (16, 128), 0)
    angle_in = jnp.zeros((16, 128), jnp.float32)
    angle_out = jnp.zeros((16, 128), jnp.float32)
    for level in range(16):
        layer = layer_ref[level]
        angle_in = jnp.where(row == level, fibre_ref[0, layer], angle_in)
        angle_out = jnp.where(row == level, fibre_ref[1, layer], angle_out)
    along_x = jnp.cos(angle_in) * jnp.cos(angle_out)
    along_y = jnp.sin(angle_in) * jnp.cos(angle_out)
    along_z = jnp.sin(angle_out)
    spread = LONGITUDINAL - TRANSVERSE
    coef[0] = TRANSVERSE + spread * along_x * along_x
    coef[1] = TRANSVERSE + spread * along_y * along_y
    coef[2] = spread * along_x * along_y / 2.0
    parts = (
        TRANSVERSE + spread * along_z * along_z,
        spread * along_x * along_z / 2.0,
        spread * along_y * along_z / 2.0,
    )
    for index, part in enumerate(parts):
        below = (part + pltpu.roll(part, 1, 0)) / 2.0
        above = (part + pltpu.roll(part, 15, 0)) / 2.0
        coef[3 + index] = jnp.where(row == 0, 0.0, below)
        coef[6 + index] = jnp.where(row == 15, 0.0, above)


def lift(tile):
    return pltpu.roll(tile, 15, 0)


def sink(tile):
    return pltpu.roll(tile, 1, 0)


def terms(coef, value, above, below):
    across = above - below
    flat = coef[1] * value
    tilt = coef[2] * across + lift(coef[5] * value) - sink(coef[8] * value)
    rest = (
        coef[0] * (above + below)
        + lift(coef[3] * value + coef[4] * across)
        + sink(coef[6] * value - coef[7] * across)
    )
    return rest, flat + tilt, flat - tilt


def plane_totals(coef, here, above, below, enter_low, enter_high):
    lane = lanes()
    first, second = (terms(coef, *tiles) for tiles in zip(here, above, below))
    after_first, after_second = pltpu.roll(first[1], 127, 1), pltpu.roll(second[1], 127, 1)
    before_first, before_second = pltpu.roll(first[2], 1, 1), pltpu.roll(second[2], 1, 1)
    low, high = lane == 0, lane == 127
    totals = (
        first[0]
        + jnp.where(high, after_second, after_first)
        + jnp.where(low, enter_low, before_first),
        second[0]
        + jnp.where(high, enter_high, after_second)
        + jnp.where(low, before_first, before_second),
    )
    return totals, first[1], second[2]


def strip_total(parts, border):
    column = lax.rem(lanes(), 16)
    after = jnp.where(column == 7, border[0], pltpu.roll(parts[1], 127, 1))
    before = jnp.where(column == 8, border[1], pltpu.roll(parts[2], 1, 1))
    return parts[0] + after + before


def kernel(
    state_ref,
    mask_ref,
    layer_ref,
    fibre_ref,
    cells,
    packed,
    keep,
    mask,
    strip_cells,
    strip_packed,
    strip_keep,
    strip_mask,
    borders,
    coef,
    hop_in,
    hop_strip_in,
    twin_in,
    twin_strip_in,
    strip_out,
    spread_out,
    spread_in,
    side_out,
    side_in,
    relay_out,
    relay_in,
    relay_gates_out,
    relay_gates_in,
    hop_send,
    hop_recv,
    strip_send,
    strip_recv,
    twin_send,
    twin_recv,
    twin_strip_send,
    twin_strip_recv,
    lead_send,
    lead_recv,
    side_send,
    side_recv,
    relay_send,
    relay_recv,
    load_sem,
):
    me_x, me_y = lax.axis_index("gx"), lax.axis_index("gy")
    size_x, size_y = lax.axis_size("gx"), lax.axis_size("gy")
    along_x = ((me_x + 1, me_y), (me_x - 1, me_y))
    along_y = ((me_x, me_y + 1), (me_x, me_y - 1))
    odd = lax.rem(me_x, 2)
    even = odd == 0
    twin = (me_x + 1 - 2 * odd, me_y)
    partner = (me_x - 1 + 2 * odd, me_y)
    has_rim = (even & (me_x > 0)) | (jnp.logical_not(even) & (me_x < size_x - 1))
    ends_x = (me_x < size_x - 1, me_x > 0)
    ends_y = (me_y < size_y - 1, me_y > 0)
    ways = (0, 1)

    def sending(ends, way, action):
        pl.when(ends[way])(action)

    def receiving(ends, way, action):
        pl.when(ends[1 - way])(action)

    barrier = pltpu.get_barrier_semaphore()
    for ends, targets in ((ends_x, along_x), (ends_y, along_y)):
        for way in ways:

            def greet(target=targets[way]):
                pl.semaphore_signal(barrier, inc=1, device_id=target, device_id_type=MESH)

            sending(ends, way, greet)

    corners = [(way_x, way_y) for way_x in ways for way_y in ways]

    def diagonal(way_x, way_y):
        return along_x[way_x][0], along_y[way_y][1]

    for way_x, way_y in corners:

        @pl.when(ends_x[way_x] & ends_y[way_y])
        def _(target=diagonal(way_x, way_y)):
            pl.semaphore_signal(barrier, inc=1, device_id=target, device_id_type=MESH)

    def remote(source, target, sends, recvs, device):
        return pltpu.make_async_remote_copy(
            src_ref=source,
            dst_ref=target,
            send_sem=sends,
            recv_sem=recvs,
            device_id=device,
            device_id_type=MESH,
        )

    def load(plane):
        return pltpu.make_async_copy(
            state_ref.at[:, plane], cells.at[:, plane + 1], load_sem.at[plane]
        )

    for plane in (0, 7, 1, 6, 2, 5, 3, 4):
        load(plane).start()

    lane = lanes()
    coefficients(layer_ref, fibre_ref, coef)
    spread_tile = jnp.zeros((16, 128), jnp.float32)
    unit = (
        lax.broadcasted_iota(jnp.int32, (16, 16), 0) == lax.broadcasted_iota(jnp.int32, (16, 16), 1)
    ).astype(jnp.float32)
    for plane in range(INNER):
        blocks = lax.dot_general(
            unit,
            (mask_ref[plane] > 0).astype(jnp.float32),
            (((1,), (1,)), ((), ())),
            preferred_element_type=jnp.float32,
        )
        for half in range(2):
            tile = jnp.broadcast_to(blocks[:, half : half + 1], (16, 128))
            mask[plane + 2, :, half * 128 : half * 128 + 128] = tile
            spread_tile = jnp.where(lane == 2 * plane + half, tile, spread_tile)
    spread_out[...] = spread_tile

    @pl.when(jnp.logical_not(has_rim))
    def _():
        for step in range(HOPS):
            hop_in[step] = jnp.zeros((16, 256), jnp.float32)
            hop_strip_in[step] = jnp.zeros((16, 128), jnp.float32)
        for comp in range(COMPS):
            cells[comp, 9 * odd] = jnp.zeros((16, 256), jnp.float32)

    for way in ways:

        @pl.when(jnp.logical_not(ends_x[1 - way]))
        def _(way=way):
            spread_in[way] = jnp.zeros((16, 128), jnp.float32)

        @pl.when(jnp.logical_not(ends_y[1 - way]))
        def _(way=way):
            for index in range(7):
                side_in[way, index] = jnp.zeros((16, 128), jnp.float32)

    for way_x, way_y in corners:

        @pl.when(jnp.logical_not(ends_x[1 - way_x] & ends_y[1 - way_y]))
        def _(slot=(way_x, way_y)):
            relay_in[slot] = jnp.zeros((16, 128), jnp.float32)
            relay_gates_in[slot] = jnp.zeros((16, 256), jnp.float32)

    def react_plane(slot, parity):
        for top in (0, 8):
            rows = pl.ds(top, 8)
            inside = mask[slot + 1, rows] > 0.0
            fresh = react([cells[comp, slot, rows] for comp in range(COMPS)], inside)
            for comp in range(COMPS):
                cells[comp, slot, rows] = fresh[comp]
            packed[parity, slot + 1, rows] = jnp.where(inside, fresh[0], 0.0)

    body = (lane >= 16) & (lane < 112)
    tips = jnp.logical_not(body)
    every = lane >= 0

    def react_strip(which, parity, region):
        for top in (0, 8):
            rows = pl.ds(top, 8)
            inside = strip_mask[which, rows] > 0.0
            fresh = react(
                [strip_cells[which, comp, rows] for comp in range(COMPS)], inside & region[0:8]
            )
            for comp in range(COMPS):
                strip_cells[which, comp, rows] = fresh[comp]
            strip_packed[parity, which, rows] = jnp.where(
                region[0:8], jnp.where(inside, fresh[0], 0.0), strip_packed[parity, which, rows]
            )

    def react_pair(pair, parity):
        react_plane(pair + 1, parity)
        react_plane(8 - pair, parity)

    def first_pair(pair, carry):
        load(pair).wait()
        load(7 - pair).wait()
        react_pair(pair, 0)
        return carry

    lax.fori_loop(0, 4, first_pair, 0)

    inner_half = lax.rem(lane, 16) < 8

    def pack_side(read):
        tile = jnp.zeros((16, 128), jnp.float32)
        for plane in range(INNER):
            first, second = read(plane)
            base = plane * 16
            both = turn(jnp.where(lane < 64, first, second), base + 8)
            tile = jnp.where((lane >= base) & (lane < base + 16), both, tile)
        return tile

    def own(comp):
        return lambda plane: (cells[comp, plane + 1, :, 0:128], cells[comp, plane + 1, :, 128:256])

    own_mask = pack_side(lambda plane: (mask[plane + 2, :, 0:128], mask[plane + 2, :, 128:256]))
    sides = [pack_side(own(0)), own_mask] + [pack_side(own(comp)) for comp in range(1, COMPS)]
    for index in range(7):
        one = sides[2 * index]
        two = sides[2 * index + 1] if index < 6 else one
        side_out[0, index] = jnp.where(inner_half, one, turn(two, 8))
        side_out[1, index] = jnp.where(inner_half, turn(two, -8), one)
    for way, (edge, inward) in enumerate(((7, 6), (0, 1))):
        tile = jnp.zeros((16, 128), jnp.float32)
        parts = (
            (sides[0], edge),
            (own_mask, edge),
            (own_mask, inward),
            (sides[0] * own_mask, inward),
        )
        for group, (part, plane) in enumerate(parts):
            here = (lane >= group * 16) & (lane < group * 16 + 16)
            tile = jnp.where(here, turn(part, group * 16 - plane * 16), tile)
        relay_out[way] = tile
        for half, gates in enumerate((range(1, 9), range(9, 12))):
            tile = jnp.zeros((16, 128), jnp.float32)
            for group, comp in enumerate(gates):
                here = (lane >= group * 16) & (lane < group * 16 + 16)
                tile = jnp.where(here, turn(sides[comp + 1], group * 16 - edge * 16), tile)
            relay_gates_out[way, :, half * 128 : half * 128 + 128] = tile

    peers_x = sum(end.astype(jnp.int32) for end in ends_x)
    peers_y = sum(end.astype(jnp.int32) for end in ends_y)
    peers = peers_x + peers_y + peers_x * peers_y
    pl.semaphore_wait(barrier, peers)

    early, late, lead = [], [], []
    for way in ways:
        early.append(
            remote(
                side_out.at[way, 0],
                side_in.at[way, 0],
                side_send.at[0, way],
                side_recv.at[0, way],
                along_y[way],
            )
        )
        late.append(
            remote(
                side_out.at[way, pl.ds(1, 6)],
                side_in.at[way, pl.ds(1, 6)],
                side_send.at[1, way],
                side_recv.at[1, way],
                along_y[way],
            )
        )
        lead.append(
            remote(
                spread_out,
                spread_in.at[way],
                lead_send.at[0, way],
                lead_recv.at[0, way],
                along_x[way],
            )
        )

    def rim_copy(index):
        source, target = (
            (cells.at[0, 1 + 7 * odd], cells.at[0, 9 - 9 * odd]),
            (packed.at[0, 3 + 5 * odd], hop_in.at[0]),
            (cells.at[pl.ds(1, 11), 1 + 7 * odd], cells.at[pl.ds(1, 11), 9 - 9 * odd]),
        )[index]
        return remote(
            source, target, lead_send.at[index + 1, 0], lead_recv.at[index + 1, 0], partner
        )

    def rim_action(action):
        pl.when(has_rim)(action)

    def twin_hop(step, parity):
        return remote(
            packed.at[parity, 9 - 7 * odd],
            twin_in.at[step],
            twin_send.at[step],
            twin_recv.at[step],
            twin,
        )

    def twin_strip_hop(step, parity):
        return remote(
            strip_packed.at[parity, 0],
            twin_strip_in.at[step],
            twin_strip_send.at[step],
            twin_strip_recv.at[step],
            twin,
        )

    def corner_copy(way_x, way_y, index):
        source, target = ((relay_out, relay_in), (relay_gates_out, relay_gates_in))[index]
        return remote(
            source.at[way_x],
            target.at[way_x, way_y],
            relay_send.at[index, way_x, way_y],
            relay_recv.at[index, way_x, way_y],
            diagonal(way_x, way_y),
        )

    def corner_start(index):
        for way_x, way_y in corners:

            @pl.when(ends_x[way_x] & ends_y[way_y])
            def _(way_x=way_x, way_y=way_y):
                corner_copy(way_x, way_y, index).start()

    def corner_sent(index):
        for way_x, way_y in corners:

            @pl.when(ends_x[way_x] & ends_y[way_y])
            def _(way_x=way_x, way_y=way_y):
                corner_copy(way_x, way_y, index).wait_send()

    def corner_wait(index):
        for way_x, way_y in corners:

            @pl.when(ends_x[1 - way_x] & ends_y[1 - way_y])
            def _(way_x=way_x, way_y=way_y):
                corner_copy(way_x, way_y, index).wait_recv()

    corner_start(0)
    for way in ways:
        sending(ends_y, way, early[way].start)
    rim_action(rim_copy(0).start)
    rim_action(rim_copy(1).start)
    for way in ways:
        sending(ends_x, way, lead[way].start)
    twin_hop(0, 0).start()
    for way in ways:
        sending(ends_y, way, late[way].start)
    corner_start(1)
    rim_action(rim_copy(2).start)

    def unpack(index):
        one = jnp.where(inner_half, side_in[0, index], side_in[1, index])
        two = jnp.where(inner_half, turn(side_in[0, index], -8), turn(side_in[1, index], 8))
        return one, two

    for way in ways:
        receiving(ends_y, way, early[way].wait_recv)
    strip_cells[0, 0], strip_mask[0] = unpack(0)
    strip_packed[0, 0] = strip_mask[0] * strip_cells[0, 0]

    def load_factors():
        return [coef[index] for index in range(9)]

    def sum_planes(factors, read, planes, parts, border, emit):
        leave_low, leave_high = border
        for plane in planes:
            base = 16 * plane
            totals, low, high = plane_totals(
                factors,
                read(plane),
                read(plane + 1),
                read(plane - 1),
                turn(parts[2], -(base + 7)),
                turn(parts[1], 127 - (base + 8)),
            )
            for half in range(2):
                emit(plane, half, totals[half])
            leave_low = jnp.where(lane == base + 7, turn(low, base + 7), leave_low)
            leave_high = jnp.where(lane == base + 8, turn(high, base + 9), leave_high)
        return leave_low, leave_high

    empty = jnp.zeros((16, 128), jnp.float32)

    def inner_sums(read, strip, kept, emit):
        factors = load_factors()
        parts = terms(factors, strip, turn(strip, 112), turn(strip, 16))
        planes = range(2, INNER - 2)
        border = sum_planes(factors, read, planes, parts, (empty, empty), emit)
        for index, tile in enumerate(border):
            borders[kept, index] = tile

    def middle_sums(read, strip, kept, emit, emit_strip):
        factors = load_factors()
        parts = terms(factors, strip, turn(strip, 112), turn(strip, 16))
        planes = (1, INNER - 2)
        border = borders[kept, 0], borders[kept, 1]
        border = sum_planes(factors, read, planes, parts, border, emit)
        emit_strip(strip_total(parts, border))

    def edge_sums(read, strips, emit, emit_strip):
        factors = load_factors()
        strip, outer = strips
        above = jnp.where(lane >= 112, turn(outer, 96), turn(strip, 112))
        below = jnp.where(lane < 16, outer, turn(strip, 16))
        parts = terms(factors, strip, above, below)
        planes = (0, INNER - 1)
        border = sum_planes(factors, read, planes, parts, (empty, empty), emit)
        if emit_strip is not None:
            emit_strip(strip_total(parts, border))

    def rim_sums(read, strips, far, beyond, emit, emit_strip):
        factors = load_factors()
        strip, outer = strips
        lower = lane < 16
        near_strip = jnp.where(lower, strip, turn(strip, 32))
        parts = terms(
            factors,
            outer,
            jnp.where(lower, near_strip, beyond),
            jnp.where(lower, beyond, near_strip),
        )
        near = read(7 * odd)
        above = [jnp.where(even, a, b) for a, b in zip(near, far)]
        below = [jnp.where(even, b, a) for a, b in zip(near, far)]
        totals, low, high = plane_totals(
            factors,
            read(9 * odd - 1),
            above,
            below,
            jnp.where(even, turn(parts[2], -7), turn(parts[2], -23)),
            jnp.where(even, turn(parts[1], 119), turn(parts[1], 103)),
        )
        for half in range(2):
            emit(9 * odd - 1, half, totals[half])
        leave_low = jnp.where(lane == 7, turn(low, 7), turn(low, 23))
        leave_high = jnp.where(lane == 8, turn(high, 9), turn(high, 25))
        emit_strip(strip_total(parts, (leave_low, leave_high)))

    def mask_tiles(plane):
        return mask[plane + 2, :, 0:128], mask[plane + 2, :, 128:256]

    def keep_plane(plane, half, total):
        columns = slice(half * 128, half * 128 + 128)
        keep[plane + 1, :, columns] = 1.0 - mask[plane + 2, :, columns] * total

    def keep_strip(which, region):
        def emit(total):
            strip_keep[which] = jnp.where(
                region, 1.0 - strip_mask[which] * total, strip_keep[which]
            )

        return emit

    def move_plane(plane, half, total):
        columns = slice(half * 128, half * 128 + 128)
        cells[0, plane + 1, :, columns] = (
            cells[0, plane + 1, :, columns] * keep[plane + 1, :, columns]
            + mask[plane + 2, :, columns] * total
        )

    def move_strip(which, region):
        def emit(total):
            value = strip_cells[which, 0]
            moved = value * strip_keep[which] + strip_mask[which] * total
            strip_cells[which, 0] = jnp.where(region, moved, value)

        return emit

    def tiles(parity):
        return lambda plane: (
            packed[parity, plane + 2, :, 0:128],
            packed[parity, plane + 2, :, 128:256],
        )

    def strips_of(parity):
        return strip_packed[parity, 0], strip_packed[parity, 1]

    def hop(step, parity):
        return remote(
            packed.at[parity, 3 + 5 * odd],
            hop_in.at[step],
            hop_send.at[step],
            hop_recv.at[step],
            partner,
        )

    def strip_hop(step, parity):
        return remote(
            strip_out.at[parity],
            hop_strip_in.at[step],
            strip_send.at[step],
            strip_recv.at[step],
            partner,
        )

    rim_lanes = (lane >= 16 * odd) & (lane < 16 * odd + 16)
    twin_lanes = (lane >= 16 - 16 * odd) & (lane < 32 - 16 * odd)

    def rim_step(step, parity):
        far = hop_in[step - 1, :, 0:128], hop_in[step - 1, :, 128:256]
        strip = hop_strip_in[step - 1]
        beyond = jnp.where(even, turn(strip, 32), strip)
        rim_sums(
            tiles(parity), strips_of(parity), far, beyond, move_plane, move_strip(1, rim_lanes)
        )

    def take_twin(step, parity):
        twin_hop(step, parity).wait_recv()
        twin_strip_hop(step, parity).wait_recv()
        packed[parity, 10 - 9 * odd] = twin_in[step]
        strip_packed[parity, 1] = jnp.where(
            twin_lanes, turn(twin_strip_in[step], 16), strip_packed[parity, 1]
        )

    def open_rim():
        corner_wait(0)
        for way in ways:
            receiving(ends_x, way, lead[way].wait_recv)
        rim_action(rim_copy(0).wait_recv)
        rim_action(rim_copy(1).wait_recv)
        twin_hop(0, 0).wait_recv()
        moved = []
        outer_mask = jnp.zeros((16, 128), jnp.float32)
        outer_far_mask = jnp.zeros((16, 128), jnp.float32)
        outer_first = jnp.zeros((16, 128), jnp.float32)
        for way, (edge, inward, slot, beyond) in enumerate(((7, 6, 1, 0), (0, 1, 10, 11))):
            for half in range(2):
                columns = slice(half * 128, half * 128 + 128)
                for plane, target in ((edge, slot), (inward, beyond)):
                    index = 2 * plane + half
                    mask[target, :, columns] = jnp.broadcast_to(
                        spread_in[way, :, index : index + 1], (16, 128)
                    )
            place = way * 16
            here = (lane >= place) & (lane < place + 16)
            relayed = jnp.where(inner_half, relay_in[way, 0], relay_in[way, 1])
            outer_first = jnp.where(here, turn(relayed, place), outer_first)
            outer_mask = jnp.where(here, turn(relayed, place - 16), outer_mask)
            outer_far_mask = jnp.where(here, turn(relayed, place - 32), outer_far_mask)
            moved.append(turn(relayed, inward * 16 - 48))
        rim_slot = 9 * odd
        packed[0, rim_slot + 1] = mask[rim_slot + 1] * cells[0, rim_slot]
        packed[0, 10 - rim_slot] = twin_in[0]
        hop_strip_in[0] = jnp.where(even, moved[0], moved[1])
        strip_cells[1, 0] = outer_first
        strip_mask[1] = outer_mask
        strip_packed[0, 1] = outer_mask * outer_first
        strip_packed[1, 1] = empty
        masks = (strip_mask[0], outer_mask)
        edge_sums(mask_tiles, masks, keep_plane, keep_strip(0, tips))
        far = mask[11 * odd, :, 0:128], mask[11 * odd, :, 128:256]
        rim_sums(mask_tiles, masks, far, outer_far_mask, keep_plane, keep_strip(1, every))

    def open_rim_gates():
        corner_wait(1)
        rim_action(rim_copy(2).wait_recv)
        for half, gates in enumerate((range(1, 9), range(9, 12))):
            for group, comp in enumerate(gates):
                tile = jnp.zeros((16, 128), jnp.float32)
                for way in ways:
                    place = way * 16
                    here = (lane >= place) & (lane < place + 16)
                    columns = slice(half * 128, half * 128 + 128)
                    source = jnp.where(
                        inner_half,
                        relay_gates_in[way, 0, :, columns],
                        relay_gates_in[way, 1, :, columns],
                    )
                    tile = jnp.where(here, turn(source, place - group * 16), tile)
                strip_cells[1, comp] = tile

    def open_strip_gates():
        for way in ways:
            receiving(ends_y, way, late[way].wait_recv)
        for index in range(1, 7):
            one, two = unpack(index)
            strip_cells[0, 2 * index - 1] = one
            if index < 6:
                strip_cells[0, 2 * index] = two

    inner_sums(mask_tiles, strip_mask[0], 0, keep_plane)
    middle_sums(mask_tiles, strip_mask[0], 0, keep_plane, keep_strip(0, body))
    inner_sums(tiles(0), strip_packed[0, 0], 1, move_plane)

    def advance(step):
        first, second, third = (isinstance(step, int) and step == value for value in (1, 2, 3))
        ahead, done = first or second, second or third
        now = lax.rem(step, 2)
        old = 1 - now
        if not (first or second):
            rim_action(hop(step - 2, now).wait_send)
            rim_action(strip_hop(step - 2, now).wait_send)
            twin_hop(step - 2, now).wait_send()
            twin_strip_hop(step - 2, now).wait_send()
        middle_sums(tiles(old), strip_packed[old, 0], 1, move_plane, move_strip(0, body))
        if not done:
            react_pair(3, now)
        if first:
            open_strip_gates()
        react_strip(0, now, body)
        strip_out[now] = strip_packed[now, 0]
        react_pair(1, now)

        @pl.when((step < HOPS) & has_rim)
        def _():
            hop(step, now).start()
            strip_hop(step, now).start()

        if first:
            react_pair(2, now)
        if ahead:
            inner_sums(tiles(now), strip_packed[now, 0], 1, move_plane)
            react_pair(3, old)
            react_pair(2, old)
        if first:
            open_rim()
            for way in ways:
                sending(ends_x, way, lead[way].wait_send)
            for index in range(3):
                rim_action(rim_copy(index).wait_send)
            twin_hop(0, old).wait_send()
        elif second:
            open_rim_gates()
        else:
            rim_action(hop(step - 2, now).wait_recv)
            rim_action(strip_hop(step - 2, now).wait_recv)
        if not first:
            rim_step(step - 1, now)
            if not done:
                react_pair(2, now)
            react_strip(1, old, rim_lanes)
            react_plane(9 * odd, old)
            take_twin(step - 1, old)
        edge_sums(tiles(old), strips_of(old), move_plane, move_strip(0, tips))
        react_strip(0, now, tips)
        if not ahead:
            inner_sums(tiles(now), strip_packed[now, 0], 1, move_plane)
        react_pair(0, now)
        twin_hop(step, now).start()
        twin_strip_hop(step, now).start()

    advance(1)
    advance(2)
    advance(3)

    def later(step, carry):
        advance(step)
        return carry

    lax.fori_loop(4, STEPS, later, 0)

    last = (STEPS - 1) % 2
    middle_sums(tiles(last), strip_packed[last, 0], 1, move_plane, lambda total: None)
    rim_action(hop(HOPS - 1, 1 - last).wait_recv)
    rim_action(strip_hop(HOPS - 1, 1 - last).wait_recv)
    rim_step(STEPS - 1, 1 - last)
    react_strip(1, last, rim_lanes)
    react_plane(9 * odd, last)
    take_twin(STEPS - 1, last)
    edge_sums(tiles(last), strips_of(last), move_plane, None)
    corner_sent(0)
    corner_sent(1)
    rim_action(hop(HOPS - 1, 1 - last).wait_send)
    rim_action(strip_hop(HOPS - 1, 1 - last).wait_send)
    for step, parity in ((HOPS - 1, 1 - last), (HOPS, last)):
        twin_hop(step, parity).wait_send()
        twin_strip_hop(step, parity).wait_send()
    for way in ways:
        sending(ends_y, way, early[way].wait_send)
        sending(ends_y, way, late[way].wait_send)


def unload(cells, out_ref, store_sem):
    stores = [
        pltpu.make_async_copy(
            cells.at[comp, pl.ds(1, INNER)], out_ref.at[comp], store_sem.at[comp]
        )
        for comp in range(COMPS)
    ]
    for copy in stores:
        copy.start()
    for copy in stores:
        copy.wait()


def shards(state, tissue_mask, layer_index, fibre):
    vmem, sems = pltpu.VMEM, pltpu.SemaphoreType.DMA
    f32 = jnp.float32
    cells = pl.pallas_call(
        kernel,
        out_shape=vmem((COMPS, 10, 16, 256), f32),
        in_specs=[
            pl.BlockSpec(memory_space=pl.ANY),
            pl.BlockSpec(memory_space=pltpu.VMEM),
            pl.BlockSpec(memory_space=pltpu.SMEM),
            pl.BlockSpec(memory_space=pltpu.SMEM),
        ],
        out_specs=pl.BlockSpec(memory_space=pltpu.VMEM),
        scratch_shapes=[
            vmem((2, 12, 16, 256), f32),
            vmem((10, 16, 256), f32),
            vmem((12, 16, 256), f32),
            vmem((2, COMPS, 16, 128), f32),
            vmem((2, 2, 16, 128), f32),
            vmem((2, 16, 128), f32),
            vmem((2, 16, 128), f32),
            vmem((2, 2, 16, 128), f32),
            vmem((9, 16, 128), f32),
            vmem((HOPS, 16, 256), f32),
            vmem((HOPS, 16, 128), f32),
            vmem((STEPS, 16, 256), f32),
            vmem((STEPS, 16, 128), f32),
            vmem((2, 16, 128), f32),
            vmem((16, 128), f32),
            vmem((2, 16, 128), f32),
            vmem((2, 7, 16, 128), f32),
            vmem((2, 7, 16, 128), f32),
            vmem((2, 16, 128), f32),
            vmem((2, 2, 16, 128), f32),
            vmem((2, 16, 256), f32),
            vmem((2, 2, 16, 256), f32),
            sems((HOPS,)),
            sems((HOPS,)),
            sems((HOPS,)),
            sems((HOPS,)),
            sems((STEPS,)),
            sems((STEPS,)),
            sems((STEPS,)),
            sems((STEPS,)),
            sems((4, 2)),
            sems((4, 2)),
            sems((2, 2)),
            sems((2, 2)),
            sems((2, 2, 2)),
            sems((2, 2, 2)),
            sems((INNER,)),
        ],
        compiler_params=pltpu.CompilerParams(collective_id=0, has_side_effects=True, vmem_limit_bytes=64000000),
        name="slab",
    )(state, jnp.swapaxes(tissue_mask, 1, 2), layer_index, fibre)
    return pl.pallas_call(
        unload,
        out_shape=jax.ShapeDtypeStruct(state.shape, f32),
        in_specs=[pl.BlockSpec(memory_space=pl.ANY)],
        out_specs=pl.BlockSpec(memory_space=pl.ANY),
        scratch_shapes=[sems((COMPS,))],
        compiler_params=pltpu.CompilerParams(vmem_limit_bytes=1 << 20),
        name="unload",
    )(cells)


def solution(mesh):
    placed = (P(None, "gx", None, "gy"), P("gx", None, "gy"), P(), P())
    return jax.shard_map(
        shards, mesh=mesh, in_specs=placed, out_specs=P(None, "gx", None, "gy"), check_vma=False
    )
```

```python
import math

import jax
import jax.numpy as jnp
from jax import lax
from jax.experimental import pallas as pl
from jax.experimental.pallas import tpu as pltpu
from jax.sharding import PartitionSpec as P

STEPS = 8
TRANSVERSE = 0.04
LONGITUDINAL = 0.12
DT = 0.02
RTF = 8314.472 * 310.0 / 96485.3415
EK = RTF * math.log(5.4 / 138.3)
ENA = RTF * math.log(140.0 / 7.67)
EKS = RTF * math.log((5.4 + 0.03 * 140.0) / (138.3 + 0.03 * 7.67))
L2E = 1.0 / math.log(2.0)
KAPPA = -DT * L2E


def grow(volt, slope):
    return jnp.exp2(volt * (slope * L2E))


def sig(volt, centre, width):
    return jax.nn.sigmoid(volt * (1.0 / width) + (-centre / width))


def settle(gate, steady, factor):
    return steady + (gate - steady) * jnp.exp2(factor)


def membrane(s):
    x, m, h, j, d, f, r, z, p, q, w, ca = s
    v = x * 100.0
    over = v - EK
    b = grow(v, 0.05)
    ib = 1.0 / b
    b2 = b * b
    ib2 = ib * ib
    c = jnp.maximum(ca, 0.02)
    vca = (v - 0.5 * RTF * math.log(2000.0)) + (0.5 * RTF) * jnp.log(c)
    sodium = ((14.838 * m) * (m * m) * (h * j) + 0.00029) * (v - ENA)
    calcium = (0.08 * d * f + 0.000592) * vca
    sa = sig(v, EK + 200.0, -1.0 / 0.06)
    bk = (
        (30.0 * math.exp(0.0002 * (100.0 - EK))) * grow(v, 0.0002)
        + (10.0 * math.exp(0.1 * (-EK - 10.0))) * b2
    ) * sig(v, EK, 2.0)
    inward = 5.405 * sa / (sa + bk)
    potassium = (
        0.294 * r * z + 0.153 * p * q + inward + 0.0146 * sig(v, 25.0, 5.98)
    ) * over
    slow = (0.392 * w) * w * (v - EKS)
    en = grow(v, -1.0 / RTF)
    pump = (2.724 * 5.4 / 6.4 * 7.67 / 47.67) / (
        1.0 + 0.1245 * grow(v, -0.1 / RTF) + 0.0353 * en
    )
    ef = grow(v, 0.35 / RTF)
    eg = ef * en
    scale = 1000.0 / ((87.5**3 + 140.0**3) * 3.38)
    exchange = (
        (scale * 7.67**3 * 2.0) * ef - (scale * 2.5 * 140.0**3 * 0.001) * eg * c
    ) / (1.0 + 0.1 * eg)
    pump_ca = 0.1238 * c / (c + 0.5)
    total = sodium + calcium + potassium + slow + pump + exchange + pump_ca
    nx = x - (DT / 100.0) * total
    nca = ca - (DT * 0.05) * (calcium + pump_ca - 2.0 * exchange)
    low = 1.0 / (1.0 + math.exp(20.0) * grow(v, 0.5))
    nm = settle(
        m,
        sig(v, -56.86, 9.03) ** 2,
        (10.0 * KAPPA + (10.0 * KAPPA * math.exp(-12.0)) * (ib2 * ib2))
        / (sig(v, -35.0, -5.0) + sig(v, 50.0, -200.0)),
    )
    hs = sig(v, -71.55, -7.43)
    hs = hs * hs
    up = (KAPPA * 0.77 / 0.13) * sig(v, -10.66, 11.1)
    dn = (
        (KAPPA * 0.057 * math.exp(-80.0 / 6.8)) * grow(v, -1.0 / 6.8)
        + (KAPPA * 2.7) * grow(v, 0.079)
        + (KAPPA * 310000.0) * grow(v, 0.3485)
    )
    nh = settle(h, hs, up + low * (dn - up))
    up = (KAPPA * 0.6) * grow(v, 0.057) * sig(v, -32.0, 10.0)
    dn = ((KAPPA * -25428.0) * grow(v, 0.2444) - (KAPPA * 6.948e-06) * grow(v, -0.04391)) * (
        v + 37.78
    ) * sig(v, -79.23, -1.0 / 0.311) + (KAPPA * 0.02424) * grow(v, -0.01052) * sig(
        v, -40.14, 1.0 / 0.1378
    )
    nj = settle(j, hs, up + low * (dn - up))
    nd = settle(
        d,
        sig(v, -8.0, 7.5),
        KAPPA
        / ((1.96 * sig(v, -35.0, 13.0) + 0.35) * sig(v, -5.0, -5.0) + sig(v, 50.0, 20.0)),
    )
    t = v + 27.0
    nf = settle(
        f,
        sig(v, -20.0, -7.0),
        1.0
        / (
            (1102.5 / KAPPA) * jnp.exp2(t * t * (-L2E / 225.0))
            + (200.0 / KAPPA) * sig(v, 13.0, 10.0)
            + (180.0 / KAPPA) * sig(v, -30.0, -10.0)
            + 20.0 / KAPPA
        ),
    )
    t = v + 40.0
    nr = settle(
        r,
        sig(v, 20.0, 6.0),
        1.0 / ((9.5 / KAPPA) * jnp.exp2(t * t * (-L2E / 1800.0)) + 0.8 / KAPPA),
    )
    t = v + 45.0
    nz = settle(
        z,
        sig(v, -20.0, -5.0),
        1.0
        / (
            (85.0 / KAPPA) * jnp.exp2(t * t * (-L2E / 320.0))
            + (5.0 / KAPPA) * sig(v, 20.0, -5.0)
            + 3.0 / KAPPA
        ),
    )
    k = KAPPA / 2700.0
    np_ = settle(
        p,
        sig(v, -26.0, 7.0),
        (k + (k * math.exp(-4.5)) * ib2)
        * (1.0 + math.exp(30.0 / 11.5) * grow(v, 1.0 / 11.5)),
    )
    k = KAPPA / 3.36
    nq = settle(
        q,
        sig(v, -88.0, -24.0),
        (k * (1.0 + math.exp(-6.0))) + (k * math.exp(-3.0)) * (b + ib),
    )
    nw = settle(
        w,
        sig(v, -5.0, 14.0),
        1.0
        / (
            lax.rsqrt(1.0 + math.exp(5.0 / 6.0) * grow(v, -1.0 / 6.0))
            * ((1400.0 / KAPPA) * sig(v, 35.0, -15.0))
            + 80.0 / KAPPA
        ),
    )
    return nx, nm, nh, nj, nd, nf, nr, nz, np_, nq, nw, nca


INNER = 8
COMPS = 12
HOPS = STEPS - 1
MESH = pl.DeviceIdType.MESH


def react(state, inside):
    fresh = membrane(state)
    return [jnp.where(inside, new, old) for new, old in zip(fresh, state)]


def lanes():
    return lax.broadcasted_iota(jnp.int32, (16, 128), 1)


def turn(tile, shift):
    shift = shift % 128
    return tile if shift == 0 else pltpu.roll(tile, shift, 1)


def coefficients(layer_ref, fibre_ref, coef):
    row = lax.broadcasted_iota(jnp.int32, (16, 128), 0)
    angle_in = jnp.zeros((16, 128), jnp.float32)
    angle_out = jnp.zeros((16, 128), jnp.float32)
    for level in range(16):
        layer = layer_ref[level]
        angle_in = jnp.where(row == level, fibre_ref[0, layer], angle_in)
        angle_out = jnp.where(row == level, fibre_ref[1, layer], angle_out)
    along_x = jnp.cos(angle_in) * jnp.cos(angle_out)
    along_y = jnp.sin(angle_in) * jnp.cos(angle_out)
    along_z = jnp.sin(angle_out)
    spread = LONGITUDINAL - TRANSVERSE
    coef[0] = TRANSVERSE + spread * along_x * along_x
    coef[1] = TRANSVERSE + spread * along_y * along_y
    coef[2] = spread * along_x * along_y / 2.0
    parts = (
        TRANSVERSE + spread * along_z * along_z,
        spread * along_x * along_z / 2.0,
        spread * along_y * along_z / 2.0,
    )
    for index, part in enumerate(parts):
        below = (part + pltpu.roll(part, 1, 0)) / 2.0
        above = (part + pltpu.roll(part, 15, 0)) / 2.0
        coef[3 + index] = jnp.where(row == 0, 0.0, below)
        coef[6 + index] = jnp.where(row == 15, 0.0, above)


def lift(tile):
    return pltpu.roll(tile, 15, 0)


def sink(tile):
    return pltpu.roll(tile, 1, 0)


def terms(coef, value, above, below):
    across = above - below
    flat = coef[1] * value
    tilt = coef[2] * across + lift(coef[5] * value) - sink(coef[8] * value)
    rest = (
        coef[0] * (above + below)
        + lift(coef[3] * value + coef[4] * across)
        + sink(coef[6] * value - coef[7] * across)
    )
    return rest, flat + tilt, flat - tilt


def plane_totals(coef, here, above, below, enter_low, enter_high):
    lane = lanes()
    first, second = (terms(coef, *tiles) for tiles in zip(here, above, below))
    after_first, after_second = pltpu.roll(first[1], 127, 1), pltpu.roll(second[1], 127, 1)
    before_first, before_second = pltpu.roll(first[2], 1, 1), pltpu.roll(second[2], 1, 1)
    low, high = lane == 0, lane == 127
    totals = (
        first[0]
        + jnp.where(high, after_second, after_first)
        + jnp.where(low, enter_low, before_first),
        second[0]
        + jnp.where(high, enter_high, after_second)
        + jnp.where(low, before_first, before_second),
    )
    return totals, first[1], second[2]


def strip_total(parts, border):
    column = lax.rem(lanes(), 16)
    after = jnp.where(column == 7, border[0], pltpu.roll(parts[1], 127, 1))
    before = jnp.where(column == 8, border[1], pltpu.roll(parts[2], 1, 1))
    return parts[0] + after + before


def kernel(
    state_ref,
    mask_ref,
    layer_ref,
    fibre_ref,
    cells,
    packed,
    keep,
    mask,
    strip_cells,
    strip_packed,
    strip_keep,
    strip_mask,
    borders,
    coef,
    hop_in,
    hop_strip_in,
    twin_in,
    twin_strip_in,
    strip_out,
    spread_out,
    spread_in,
    side_out,
    side_in,
    relay_out,
    relay_in,
    relay_gates_out,
    relay_gates_in,
    hop_send,
    hop_recv,
    strip_send,
    strip_recv,
    twin_send,
    twin_recv,
    twin_strip_send,
    twin_strip_recv,
    lead_send,
    lead_recv,
    side_send,
    side_recv,
    relay_send,
    relay_recv,
    load_sem,
):
    me_x, me_y = lax.axis_index("gx"), lax.axis_index("gy")
    size_x, size_y = lax.axis_size("gx"), lax.axis_size("gy")
    along_x = ((me_x + 1, me_y), (me_x - 1, me_y))
    along_y = ((me_x, me_y + 1), (me_x, me_y - 1))
    odd = lax.rem(me_x, 2)
    even = odd == 0
    twin = (me_x + 1 - 2 * odd, me_y)
    partner = (me_x - 1 + 2 * odd, me_y)
    has_rim = (even & (me_x > 0)) | (jnp.logical_not(even) & (me_x < size_x - 1))
    ends_x = (me_x < size_x - 1, me_x > 0)
    ends_y = (me_y < size_y - 1, me_y > 0)
    ways = (0, 1)

    def sending(ends, way, action):
        pl.when(ends[way])(action)

    def receiving(ends, way, action):
        pl.when(ends[1 - way])(action)

    barrier = pltpu.get_barrier_semaphore()
    for ends, targets in ((ends_x, along_x), (ends_y, along_y)):
        for way in ways:

            def greet(target=targets[way]):
                pl.semaphore_signal(barrier, inc=1, device_id=target, device_id_type=MESH)

            sending(ends, way, greet)

    corners = [(way_x, way_y) for way_x in ways for way_y in ways]

    def diagonal(way_x, way_y):
        return along_x[way_x][0], along_y[way_y][1]

    for way_x, way_y in corners:

        @pl.when(ends_x[way_x] & ends_y[way_y])
        def _(target=diagonal(way_x, way_y)):
            pl.semaphore_signal(barrier, inc=1, device_id=target, device_id_type=MESH)

    def remote(source, target, sends, recvs, device):
        return pltpu.make_async_remote_copy(
            src_ref=source,
            dst_ref=target,
            send_sem=sends,
            recv_sem=recvs,
            device_id=device,
            device_id_type=MESH,
        )

    def load(plane):
        return pltpu.make_async_copy(
            state_ref.at[:, plane], cells.at[:, plane + 1], load_sem.at[plane]
        )

    for plane in (0, 7, 1, 6, 2, 5, 3, 4):
        load(plane).start()

    lane = lanes()
    coefficients(layer_ref, fibre_ref, coef)
    spread_tile = jnp.zeros((16, 128), jnp.float32)
    unit = (
        lax.broadcasted_iota(jnp.int32, (16, 16), 0) == lax.broadcasted_iota(jnp.int32, (16, 16), 1)
    ).astype(jnp.float32)
    for plane in range(INNER):
        blocks = lax.dot_general(
            unit,
            (mask_ref[plane] > 0).astype(jnp.float32),
            (((1,), (1,)), ((), ())),
            preferred_element_type=jnp.float32,
        )
        for half in range(2):
            tile = jnp.broadcast_to(blocks[:, half : half + 1], (16, 128))
            mask[plane + 2, :, half * 128 : half * 128 + 128] = tile
            spread_tile = jnp.where(lane == 2 * plane + half, tile, spread_tile)
    spread_out[...] = spread_tile

    @pl.when(jnp.logical_not(has_rim))
    def _():
        for step in range(HOPS):
            hop_in[step] = jnp.zeros((16, 256), jnp.float32)
            hop_strip_in[step] = jnp.zeros((16, 128), jnp.float32)
        for comp in range(COMPS):
            cells[comp, 9 * odd] = jnp.zeros((16, 256), jnp.float32)

    for way in ways:

        @pl.when(jnp.logical_not(ends_x[1 - way]))
        def _(way=way):
            spread_in[way] = jnp.zeros((16, 128), jnp.float32)

        @pl.when(jnp.logical_not(ends_y[1 - way]))
        def _(way=way):
            for index in range(7):
                side_in[way, index] = jnp.zeros((16, 128), jnp.float32)

    for way_x, way_y in corners:

        @pl.when(jnp.logical_not(ends_x[1 - way_x] & ends_y[1 - way_y]))
        def _(slot=(way_x, way_y)):
            relay_in[slot] = jnp.zeros((16, 128), jnp.float32)
            relay_gates_in[slot] = jnp.zeros((16, 256), jnp.float32)

    def react_plane(slot, parity):
        for top in (0, 8):
            rows = pl.ds(top, 8)
            inside = mask[slot + 1, rows] > 0.0
            fresh = react([cells[comp, slot, rows] for comp in range(COMPS)], inside)
            for comp in range(COMPS):
                cells[comp, slot, rows] = fresh[comp]
            packed[parity, slot + 1, rows] = jnp.where(inside, fresh[0], 0.0)

    body = (lane >= 16) & (lane < 112)
    tips = jnp.logical_not(body)
    every = lane >= 0

    def react_strip(which, parity, region):
        for top in (0, 8):
            rows = pl.ds(top, 8)
            inside = strip_mask[which, rows] > 0.0
            fresh = react(
                [strip_cells[which, comp, rows] for comp in range(COMPS)], inside & region[0:8]
            )
            for comp in range(COMPS):
                strip_cells[which, comp, rows] = fresh[comp]
            strip_packed[parity, which, rows] = jnp.where(
                region[0:8], jnp.where(inside, fresh[0], 0.0), strip_packed[parity, which, rows]
            )

    def react_pair(pair, parity):
        react_plane(pair + 1, parity)
        react_plane(8 - pair, parity)

    def first_pair(pair, carry):
        load(pair).wait()
        load(7 - pair).wait()
        react_pair(pair, 0)
        return carry

    lax.fori_loop(0, 4, first_pair, 0)

    inner_half = lax.rem(lane, 16) < 8

    def pack_side(read):
        tile = jnp.zeros((16, 128), jnp.float32)
        for plane in range(INNER):
            first, second = read(plane)
            base = plane * 16
            both = turn(jnp.where(lane < 64, first, second), base + 8)
            tile = jnp.where((lane >= base) & (lane < base + 16), both, tile)
        return tile

    def own(comp):
        return lambda plane: (cells[comp, plane + 1, :, 0:128], cells[comp, plane + 1, :, 128:256])

    own_mask = pack_side(lambda plane: (mask[plane + 2, :, 0:128], mask[plane + 2, :, 128:256]))
    sides = [pack_side(own(0)), own_mask] + [pack_side(own(comp)) for comp in range(1, COMPS)]
    for index in range(7):
        one = sides[2 * index]
        two = sides[2 * index + 1] if index < 6 else one
        side_out[0, index] = jnp.where(inner_half, one, turn(two, 8))
        side_out[1, index] = jnp.where(inner_half, turn(two, -8), one)
    for way, (edge, inward) in enumerate(((7, 6), (0, 1))):
        tile = jnp.zeros((16, 128), jnp.float32)
        parts = (
            (sides[0], edge),
            (own_mask, edge),
            (own_mask, inward),
            (sides[0] * own_mask, inward),
        )
        for group, (part, plane) in enumerate(parts):
            here = (lane >= group * 16) & (lane < group * 16 + 16)
            tile = jnp.where(here, turn(part, group * 16 - plane * 16), tile)
        relay_out[way] = tile
        for half, gates in enumerate((range(1, 9), range(9, 12))):
            tile = jnp.zeros((16, 128), jnp.float32)
            for group, comp in enumerate(gates):
                here = (lane >= group * 16) & (lane < group * 16 + 16)
                tile = jnp.where(here, turn(sides[comp + 1], group * 16 - edge * 16), tile)
            relay_gates_out[way, :, half * 128 : half * 128 + 128] = tile

    peers_x = sum(end.astype(jnp.int32) for end in ends_x)
    peers_y = sum(end.astype(jnp.int32) for end in ends_y)
    peers = peers_x + peers_y + peers_x * peers_y
    pl.semaphore_wait(barrier, peers)

    early, late, lead = [], [], []
    for way in ways:
        early.append(
            remote(
                side_out.at[way, 0],
                side_in.at[way, 0],
                side_send.at[0, way],
                side_recv.at[0, way],
                along_y[way],
            )
        )
        late.append(
            remote(
                side_out.at[way, pl.ds(1, 6)],
                side_in.at[way, pl.ds(1, 6)],
                side_send.at[1, way],
                side_recv.at[1, way],
                along_y[way],
            )
        )
        lead.append(
            remote(
                spread_out,
                spread_in.at[way],
                lead_send.at[0, way],
                lead_recv.at[0, way],
                along_x[way],
            )
        )

    def rim_copy(index):
        source, target = (
            (cells.at[0, 1 + 7 * odd], cells.at[0, 9 - 9 * odd]),
            (packed.at[0, 3 + 5 * odd], hop_in.at[0]),
            (cells.at[pl.ds(1, 11), 1 + 7 * odd], cells.at[pl.ds(1, 11), 9 - 9 * odd]),
        )[index]
        return remote(
            source, target, lead_send.at[index + 1, 0], lead_recv.at[index + 1, 0], partner
        )

    def rim_action(action):
        pl.when(has_rim)(action)

    def twin_hop(step, parity):
        return remote(
            packed.at[parity, 9 - 7 * odd],
            twin_in.at[step],
            twin_send.at[step],
            twin_recv.at[step],
            twin,
        )

    def twin_strip_hop(step, parity):
        return remote(
            strip_packed.at[parity, 0],
            twin_strip_in.at[step],
            twin_strip_send.at[step],
            twin_strip_recv.at[step],
            twin,
        )

    def corner_copy(way_x, way_y, index):
        source, target = ((relay_out, relay_in), (relay_gates_out, relay_gates_in))[index]
        return remote(
            source.at[way_x],
            target.at[way_x, way_y],
            relay_send.at[index, way_x, way_y],
            relay_recv.at[index, way_x, way_y],
            diagonal(way_x, way_y),
        )

    def corner_start(index):
        for way_x, way_y in corners:

            @pl.when(ends_x[way_x] & ends_y[way_y])
            def _(way_x=way_x, way_y=way_y):
                corner_copy(way_x, way_y, index).start()

    def corner_sent(index):
        for way_x, way_y in corners:

            @pl.when(ends_x[way_x] & ends_y[way_y])
            def _(way_x=way_x, way_y=way_y):
                corner_copy(way_x, way_y, index).wait_send()

    def corner_wait(index):
        for way_x, way_y in corners:

            @pl.when(ends_x[1 - way_x] & ends_y[1 - way_y])
            def _(way_x=way_x, way_y=way_y):
                corner_copy(way_x, way_y, index).wait_recv()

    corner_start(0)
    for way in ways:
        sending(ends_y, way, early[way].start)
    rim_action(rim_copy(0).start)
    for way in ways:
        sending(ends_x, way, lead[way].start)
    twin_hop(0, 0).start()
    for way in ways:
        sending(ends_y, way, late[way].start)
    rim_action(rim_copy(2).start)
    corner_start(1)
    rim_action(rim_copy(1).start)

    def unpack(index):
        one = jnp.where(inner_half, side_in[0, index], side_in[1, index])
        two = jnp.where(inner_half, turn(side_in[0, index], -8), turn(side_in[1, index], 8))
        return one, two

    for way in ways:
        receiving(ends_y, way, early[way].wait_recv)
    strip_cells[0, 0], strip_mask[0] = unpack(0)
    strip_packed[0, 0] = strip_mask[0] * strip_cells[0, 0]

    def load_factors():
        return [coef[index] for index in range(9)]

    def sum_planes(factors, read, planes, parts, border, emit):
        leave_low, leave_high = border
        for plane in planes:
            base = 16 * plane
            totals, low, high = plane_totals(
                factors,
                read(plane),
                read(plane + 1),
                read(plane - 1),
                turn(parts[2], -(base + 7)),
                turn(parts[1], 127 - (base + 8)),
            )
            for half in range(2):
                emit(plane, half, totals[half])
            leave_low = jnp.where(lane == base + 7, turn(low, base + 7), leave_low)
            leave_high = jnp.where(lane == base + 8, turn(high, base + 9), leave_high)
        return leave_low, leave_high

    empty = jnp.zeros((16, 128), jnp.float32)

    def inner_sums(read, strip, kept, emit):
        factors = load_factors()
        parts = terms(factors, strip, turn(strip, 112), turn(strip, 16))
        planes = range(2, INNER - 2)
        border = sum_planes(factors, read, planes, parts, (empty, empty), emit)
        for index, tile in enumerate(border):
            borders[kept, index] = tile

    def middle_sums(read, strip, kept, emit, emit_strip):
        factors = load_factors()
        parts = terms(factors, strip, turn(strip, 112), turn(strip, 16))
        planes = (1, INNER - 2)
        border = borders[kept, 0], borders[kept, 1]
        border = sum_planes(factors, read, planes, parts, border, emit)
        emit_strip(strip_total(parts, border))

    def edge_sums(read, strips, emit, emit_strip):
        factors = load_factors()
        strip, outer = strips
        above = jnp.where(lane >= 112, turn(outer, 96), turn(strip, 112))
        below = jnp.where(lane < 16, outer, turn(strip, 16))
        parts = terms(factors, strip, above, below)
        planes = (0, INNER - 1)
        border = sum_planes(factors, read, planes, parts, (empty, empty), emit)
        if emit_strip is not None:
            emit_strip(strip_total(parts, border))

    def rim_sums(read, strips, far, beyond, emit, emit_strip):
        factors = load_factors()
        strip, outer = strips
        lower = lane < 16
        near_strip = jnp.where(lower, strip, turn(strip, 32))
        parts = terms(
            factors,
            outer,
            jnp.where(lower, near_strip, beyond),
            jnp.where(lower, beyond, near_strip),
        )
        near = read(7 * odd)
        above = [jnp.where(even, a, b) for a, b in zip(near, far)]
        below = [jnp.where(even, b, a) for a, b in zip(near, far)]
        totals, low, high = plane_totals(
            factors,
            read(9 * odd - 1),
            above,
            below,
            jnp.where(even, turn(parts[2], -7), turn(parts[2], -23)),
            jnp.where(even, turn(parts[1], 119), turn(parts[1], 103)),
        )
        for half in range(2):
            emit(9 * odd - 1, half, totals[half])
        leave_low = jnp.where(lane == 7, turn(low, 7), turn(low, 23))
        leave_high = jnp.where(lane == 8, turn(high, 9), turn(high, 25))
        emit_strip(strip_total(parts, (leave_low, leave_high)))

    def mask_tiles(plane):
        return mask[plane + 2, :, 0:128], mask[plane + 2, :, 128:256]

    def keep_plane(plane, half, total):
        columns = slice(half * 128, half * 128 + 128)
        keep[plane + 1, :, columns] = 1.0 - mask[plane + 2, :, columns] * total

    def keep_strip(which, region):
        def emit(total):
            strip_keep[which] = jnp.where(
                region, 1.0 - strip_mask[which] * total, strip_keep[which]
            )

        return emit

    def move_plane(plane, half, total):
        columns = slice(half * 128, half * 128 + 128)
        cells[0, plane + 1, :, columns] = (
            cells[0, plane + 1, :, columns] * keep[plane + 1, :, columns]
            + mask[plane + 2, :, columns] * total
        )

    def move_strip(which, region):
        def emit(total):
            value = strip_cells[which, 0]
            moved = value * strip_keep[which] + strip_mask[which] * total
            strip_cells[which, 0] = jnp.where(region, moved, value)

        return emit

    def tiles(parity):
        return lambda plane: (
            packed[parity, plane + 2, :, 0:128],
            packed[parity, plane + 2, :, 128:256],
        )

    def strips_of(parity):
        return strip_packed[parity, 0], strip_packed[parity, 1]

    def hop(step, parity):
        return remote(
            packed.at[parity, 3 + 5 * odd],
            hop_in.at[step],
            hop_send.at[step],
            hop_recv.at[step],
            partner,
        )

    def strip_hop(step, parity):
        return remote(
            strip_out.at[parity],
            hop_strip_in.at[step],
            strip_send.at[step],
            strip_recv.at[step],
            partner,
        )

    rim_lanes = (lane >= 16 * odd) & (lane < 16 * odd + 16)
    twin_lanes = (lane >= 16 - 16 * odd) & (lane < 32 - 16 * odd)

    def rim_step(step, parity):
        far = hop_in[step - 1, :, 0:128], hop_in[step - 1, :, 128:256]
        strip = hop_strip_in[step - 1]
        beyond = jnp.where(even, turn(strip, 32), strip)
        rim_sums(
            tiles(parity), strips_of(parity), far, beyond, move_plane, move_strip(1, rim_lanes)
        )

    def take_twin(step, parity):
        twin_hop(step, parity).wait_recv()
        twin_strip_hop(step, parity).wait_recv()
        packed[parity, 10 - 9 * odd] = twin_in[step]
        strip_packed[parity, 1] = jnp.where(
            twin_lanes, turn(twin_strip_in[step], 16), strip_packed[parity, 1]
        )

    def open_rim():
        corner_wait(0)
        for way in ways:
            receiving(ends_x, way, lead[way].wait_recv)
        rim_action(rim_copy(0).wait_recv)
        twin_hop(0, 0).wait_recv()
        moved = []
        outer_mask = jnp.zeros((16, 128), jnp.float32)
        outer_far_mask = jnp.zeros((16, 128), jnp.float32)
        outer_first = jnp.zeros((16, 128), jnp.float32)
        for way, (edge, inward, slot, beyond) in enumerate(((7, 6, 1, 0), (0, 1, 10, 11))):
            for half in range(2):
                columns = slice(half * 128, half * 128 + 128)
                for plane, target in ((edge, slot), (inward, beyond)):
                    index = 2 * plane + half
                    mask[target, :, columns] = jnp.broadcast_to(
                        spread_in[way, :, index : index + 1], (16, 128)
                    )
            place = way * 16
            here = (lane >= place) & (lane < place + 16)
            relayed = jnp.where(inner_half, relay_in[way, 0], relay_in[way, 1])
            outer_first = jnp.where(here, turn(relayed, place), outer_first)
            outer_mask = jnp.where(here, turn(relayed, place - 16), outer_mask)
            outer_far_mask = jnp.where(here, turn(relayed, place - 32), outer_far_mask)
            moved.append(turn(relayed, inward * 16 - 48))
        rim_slot = 9 * odd
        packed[0, rim_slot + 1] = mask[rim_slot + 1] * cells[0, rim_slot]
        packed[0, 10 - rim_slot] = twin_in[0]
        hop_strip_in[0] = jnp.where(even, moved[0], moved[1])
        strip_cells[1, 0] = outer_first
        strip_mask[1] = outer_mask
        strip_packed[0, 1] = outer_mask * outer_first
        strip_packed[1, 1] = empty
        masks = (strip_mask[0], outer_mask)
        edge_sums(mask_tiles, masks, keep_plane, keep_strip(0, tips))
        far = mask[11 * odd, :, 0:128], mask[11 * odd, :, 128:256]
        rim_sums(mask_tiles, masks, far, outer_far_mask, keep_plane, keep_strip(1, every))

    def open_rim_gates():
        corner_wait(1)
        rim_action(rim_copy(1).wait_recv)
        rim_action(rim_copy(2).wait_recv)
        for half, gates in enumerate((range(1, 9), range(9, 12))):
            for group, comp in enumerate(gates):
                tile = jnp.zeros((16, 128), jnp.float32)
                for way in ways:
                    place = way * 16
                    here = (lane >= place) & (lane < place + 16)
                    columns = slice(half * 128, half * 128 + 128)
                    source = jnp.where(
                        inner_half,
                        relay_gates_in[way, 0, :, columns],
                        relay_gates_in[way, 1, :, columns],
                    )
                    tile = jnp.where(here, turn(source, place - group * 16), tile)
                strip_cells[1, comp] = tile

    def open_strip_gates():
        for way in ways:
            receiving(ends_y, way, late[way].wait_recv)
        for index in range(1, 7):
            one, two = unpack(index)
            strip_cells[0, 2 * index - 1] = one
            if index < 6:
                strip_cells[0, 2 * index] = two

    inner_sums(mask_tiles, strip_mask[0], 0, keep_plane)
    middle_sums(mask_tiles, strip_mask[0], 0, keep_plane, keep_strip(0, body))
    inner_sums(tiles(0), strip_packed[0, 0], 1, move_plane)

    def advance(step):
        first, second, third = (isinstance(step, int) and step == value for value in (1, 2, 3))
        ahead, done = first or second, second or third
        now = lax.rem(step, 2)
        old = 1 - now
        if not (first or second):
            rim_action(hop(step - 2, now).wait_send)
            rim_action(strip_hop(step - 2, now).wait_send)
            twin_hop(step - 2, now).wait_send()
            twin_strip_hop(step - 2, now).wait_send()
        middle_sums(tiles(old), strip_packed[old, 0], 1, move_plane, move_strip(0, body))
        if not done:
            react_pair(3, now)
        if first:
            open_strip_gates()
        react_strip(0, now, body)
        strip_out[now] = strip_packed[now, 0]
        react_pair(1, now)

        @pl.when((step < HOPS) & has_rim)
        def _():
            hop(step, now).start()
            strip_hop(step, now).start()

        if first:
            react_pair(2, now)
        if ahead:
            inner_sums(tiles(now), strip_packed[now, 0], 1, move_plane)
            react_pair(3, old)
            react_pair(2, old)
        if first:
            open_rim()
            for way in ways:
                sending(ends_x, way, lead[way].wait_send)
            for index in range(3):
                rim_action(rim_copy(index).wait_send)
            twin_hop(0, old).wait_send()
        elif second:
            open_rim_gates()
        else:
            rim_action(hop(step - 2, now).wait_recv)
            rim_action(strip_hop(step - 2, now).wait_recv)
        if not first:
            rim_step(step - 1, now)
            if not done:
                react_pair(2, now)
            react_strip(1, old, rim_lanes)
            react_plane(9 * odd, old)
            take_twin(step - 1, old)
        edge_sums(tiles(old), strips_of(old), move_plane, move_strip(0, tips))
        react_strip(0, now, tips)
        if not ahead:
            inner_sums(tiles(now), strip_packed[now, 0], 1, move_plane)
        react_pair(0, now)
        twin_hop(step, now).start()
        twin_strip_hop(step, now).start()

    advance(1)
    advance(2)
    advance(3)

    def later(step, carry):
        advance(step)
        return carry

    lax.fori_loop(4, STEPS, later, 0)

    last = (STEPS - 1) % 2
    middle_sums(tiles(last), strip_packed[last, 0], 1, move_plane, lambda total: None)
    rim_action(hop(HOPS - 1, 1 - last).wait_recv)
    rim_action(strip_hop(HOPS - 1, 1 - last).wait_recv)
    rim_step(STEPS - 1, 1 - last)
    react_strip(1, last, rim_lanes)
    react_plane(9 * odd, last)
    take_twin(STEPS - 1, last)
    edge_sums(tiles(last), strips_of(last), move_plane, None)
    corner_sent(0)
    corner_sent(1)
    rim_action(hop(HOPS - 1, 1 - last).wait_send)
    rim_action(strip_hop(HOPS - 1, 1 - last).wait_send)
    for step, parity in ((HOPS - 1, 1 - last), (HOPS, last)):
        twin_hop(step, parity).wait_send()
        twin_strip_hop(step, parity).wait_send()
    for way in ways:
        sending(ends_y, way, early[way].wait_send)
        sending(ends_y, way, late[way].wait_send)


def unload(cells, out_ref, store_sem):
    stores = [
        pltpu.make_async_copy(
            cells.at[comp, pl.ds(1, INNER)], out_ref.at[comp], store_sem.at[comp]
        )
        for comp in range(COMPS)
    ]
    for copy in stores:
        copy.start()
    for copy in stores:
        copy.wait()


def shards(state, tissue_mask, layer_index, fibre):
    vmem, sems = pltpu.VMEM, pltpu.SemaphoreType.DMA
    f32 = jnp.float32
    cells = pl.pallas_call(
        kernel,
        out_shape=vmem((COMPS, 10, 16, 256), f32),
        in_specs=[
            pl.BlockSpec(memory_space=pl.ANY),
            pl.BlockSpec(memory_space=pltpu.VMEM),
            pl.BlockSpec(memory_space=pltpu.SMEM),
            pl.BlockSpec(memory_space=pltpu.SMEM),
        ],
        out_specs=pl.BlockSpec(memory_space=pltpu.VMEM),
        scratch_shapes=[
            vmem((2, 12, 16, 256), f32),
            vmem((10, 16, 256), f32),
            vmem((12, 16, 256), f32),
            vmem((2, COMPS, 16, 128), f32),
            vmem((2, 2, 16, 128), f32),
            vmem((2, 16, 128), f32),
            vmem((2, 16, 128), f32),
            vmem((2, 2, 16, 128), f32),
            vmem((9, 16, 128), f32),
            vmem((HOPS, 16, 256), f32),
            vmem((HOPS, 16, 128), f32),
            vmem((STEPS, 16, 256), f32),
            vmem((STEPS, 16, 128), f32),
            vmem((2, 16, 128), f32),
            vmem((16, 128), f32),
            vmem((2, 16, 128), f32),
            vmem((2, 7, 16, 128), f32),
            vmem((2, 7, 16, 128), f32),
            vmem((2, 16, 128), f32),
            vmem((2, 2, 16, 128), f32),
            vmem((2, 16, 256), f32),
            vmem((2, 2, 16, 256), f32),
            sems((HOPS,)),
            sems((HOPS,)),
            sems((HOPS,)),
            sems((HOPS,)),
            sems((STEPS,)),
            sems((STEPS,)),
            sems((STEPS,)),
            sems((STEPS,)),
            sems((4, 2)),
            sems((4, 2)),
            sems((2, 2)),
            sems((2, 2)),
            sems((2, 2, 2)),
            sems((2, 2, 2)),
            sems((INNER,)),
        ],
        compiler_params=pltpu.CompilerParams(collective_id=0, has_side_effects=True, vmem_limit_bytes=64000000),
        name="slab",
    )(state, jnp.swapaxes(tissue_mask, 1, 2), layer_index, fibre)
    return pl.pallas_call(
        unload,
        out_shape=jax.ShapeDtypeStruct(state.shape, f32),
        in_specs=[pl.BlockSpec(memory_space=pl.ANY)],
        out_specs=pl.BlockSpec(memory_space=pl.ANY),
        scratch_shapes=[sems((COMPS,))],
        compiler_params=pltpu.CompilerParams(vmem_limit_bytes=1 << 20),
        name="unload",
    )(cells)


def solution(mesh):
    placed = (P(None, "gx", None, "gy"), P("gx", None, "gy"), P(), P())
    return jax.shard_map(
        shards, mesh=mesh, in_specs=placed, out_specs=P(None, "gx", None, "gy"), check_vma=False
    )
```
